128 devices in a mesh: tm: 8 (over x, core), space: 16 (over z, y).
Axes of the slice: x: 4, y: 4, z: 4, core: 2. Of those that a mesh axis runs over, the one named last changes fastest.
Arguments:
- speed: float32 [32, 16, 128], P('space'), may hold values from 0.5 to 1.5
- forcing: float32 [32, 32, 16, 128], P('tm', 'space'), may hold values from -1.8 to 1.8
- guess: float32 [8, 4, 32, 16, 128], P('tm', None, 'space'), may hold values from -8 to 8
- basis: float32 [8, 64, 4, 32, 16, 128], P('tm', None, None, 'space'), may hold values from -1 to 1, as said below
Outputs:
- states: float32 [32, 4, 32, 16, 128], P('tm', None, 'space')
- coords: float32 [8, 64], P('tm')
The draws below stay inside these ranges and needn't reach their ends.
Inputs may be any that keep to these rules, and one draw needn't show every extreme that they name: The columns of each basis[k] are linearly independent.
All inputs are finite; a program needn't handle non-finite values.
Results may differ from the reference program's by a relative error of at most 0.00018.
Values sent between devices are 32-bit elements; how exact they have to be, the bound alone decides.
A program may use at most 128 MiB of HBM per device.

```python
import jax
import jax.numpy as jnp
from jax import lax

NX = 16
NY = 128
RANK = 64
NZ = 32
NT = 32
N_TM = 8


DT = 0.045


def shifted_ahead_drawn(values, axis):
    size = values.shape[axis]
    rest = lax.slice_in_dim(values, 1, size, axis=axis)
    border = jnp.zeros_like(lax.slice_in_dim(values, 0, 1, axis=axis))
    return jnp.concatenate([rest, border], axis=axis)


def shifted_behind_drawn(values, axis):
    size = values.shape[axis]
    rest = lax.slice_in_dim(values, 0, size - 1, axis=axis)
    border = jnp.zeros_like(lax.slice_in_dim(values, 0, 1, axis=axis))
    return jnp.concatenate([border, rest], axis=axis)


def fine_advance(state, speed_sq):
    pressure = state[..., 0, :, :, :]
    depth = pressure.ndim
    flow_x = state[..., 1, :, :, :] - DT * (shifted_ahead_drawn(pressure, depth - 2) - pressure)
    flow_y = state[..., 2, :, :, :] - DT * (shifted_ahead_drawn(pressure, depth - 1) - pressure)
    flow_z = state[..., 3, :, :, :] - DT * (shifted_ahead_drawn(pressure, depth - 3) - pressure)
    diverge = flow_x - shifted_behind_drawn(flow_x, depth - 2) + (flow_y - shifted_behind_drawn(flow_y, depth - 1)) + (flow_z - shifted_behind_drawn(flow_z, depth - 3))
    fresh = pressure - DT * speed_sq * diverge
    return jnp.stack([fresh, flow_x, flow_y, flow_z], axis=depth - 3)


def speed_field(key):
    log_speed = jax.random.uniform(jax.random.fold_in(key, 202), (NZ, NX, NY), jnp.float32, jnp.log(0.5), jnp.log(1.5))
    return jnp.clip(jnp.exp(log_speed), 0.5, 1.5)


def pattern_block(key, block_index):
    return jax.random.normal(jax.random.fold_in(jax.random.fold_in(key, 101), block_index), (RANK, 4, NZ, NX, NY), jnp.float32)


def draw_speed(key, part):
    return speed_field(key)


def draw_guess(key, part):
    mixing = jax.random.normal(jax.random.fold_in(key, 404), (N_TM, RANK), jnp.float32)

    def aligned(block_index):
        block = pattern_block(key, block_index)
        factors = mixing[block_index][:, None, None, None, None]
        return jnp.sum(factors * block, axis=0) / jnp.sqrt(jnp.float32(RANK))
    aligned_all = lax.map(aligned, jnp.arange(N_TM, dtype=jnp.int32))
    rough_part = jax.random.normal(jax.random.fold_in(key, 303), aligned_all.shape, jnp.float32)
    strength = 1.0
    return jnp.clip(rough_part + strength * aligned_all, -8.0, 8.0)


def draw_basis(key, part):
    speed_sq = jnp.square(speed_field(key))
    cell_count = 4 * NZ * NX * NY
    blend_weight = 0.0
    least_scale = 0.3
    most_scale = 3.0
    scales = jnp.exp(jax.random.uniform(jax.random.fold_in(key, 505), (N_TM, RANK), jnp.float32, jnp.log(least_scale), jnp.log(most_scale)))

    def column_block(block_index):
        source = (block_index + N_TM - 2) % N_TM
        moved_block = pattern_block(key, source)
        for repeat in range(4):
            moved_block = fine_advance(moved_block, speed_sq)
        common = jnp.sum(moved_block, axis=0) / jnp.sqrt(jnp.float32(RANK))
        mixed_columns = moved_block + blend_weight * common[None]
        column_scale = scales[block_index] / jnp.sqrt(jnp.float32(cell_count))
        return mixed_columns * column_scale[:, None, None, None, None]
    columns = lax.map(column_block, jnp.arange(N_TM, dtype=jnp.int32))
    return jnp.clip(columns, -1.0, 1.0)


def steps_of(own_key, extent, cuts, least, largest):
    level = 1.0
    for axis_at, shards_of in cuts:
        draws = jax.random.uniform(jax.random.fold_in(jax.random.fold_in(own_key, 6), axis_at), (shards_of,), jnp.float32, least / len(cuts), largest / len(cuts))
        level = level * jnp.repeat(jnp.exp(draws), extent[axis_at] // shards_of).reshape((-1,) + (1,) * (len(extent) - 1 - axis_at))
    return level


def bell_draw(own_key, shape, scale, most, cuts=(), held_as=jnp.bfloat16):
    drawn = scale * jax.random.normal(own_key, shape, jnp.float32)
    if cuts:
        drawn = drawn * steps_of(own_key, shape, cuts, -0.22, 0.18)
    return jnp.clip(drawn, -most, most).astype(held_as)


def setup_inputs(seed: int = 0) -> dict:
    key_list = jax.random.split(jax.random.key(seed), 5)
    return {
        "speed": draw_speed(jax.random.fold_in(key_list[4], 71), 0),
        "forcing": bell_draw(key_list[1], (NT, NZ, NX, NY), 0.3, 1.8, ((0, 8), (1, 16)), jnp.float32),
        "guess": draw_guess(jax.random.fold_in(key_list[4], 71), 0),
        "basis": draw_basis(jax.random.fold_in(key_list[4], 71), 0),
    }


DT = 0.045
exact_mode = lax.Precision.HIGHEST

def shifted_ahead(values, axis):
    size = values.shape[axis]
    rest = lax.slice_in_dim(values, 1, size, axis=axis)
    border = jnp.zeros_like(lax.slice_in_dim(values, 0, 1, axis=axis))
    return jnp.concatenate([rest, border], axis=axis)

def shifted_behind(values, axis):
    size = values.shape[axis]
    rest = lax.slice_in_dim(values, 0, size - 1, axis=axis)
    border = jnp.zeros_like(lax.slice_in_dim(values, 0, 1, axis=axis))
    return jnp.concatenate([border, rest], axis=axis)

def update_flow(state, upper_plane, delta_time):
    pressure = state[..., 0, :, :, :]
    depth = pressure.ndim
    above = jnp.concatenate([pressure[..., 1:, :, :], upper_plane], axis=depth - 3)
    flow_x = state[..., 1, :, :, :] - delta_time * (shifted_ahead(pressure, depth - 2) - pressure)
    flow_y = state[..., 2, :, :, :] - delta_time * (shifted_ahead(pressure, depth - 1) - pressure)
    flow_z = state[..., 3, :, :, :] - delta_time * (above - pressure)
    return (pressure, flow_x, flow_y, flow_z)

def update_pressure(pressure, flow_x, flow_y, flow_z, lower_plane, speed_sq, delta_time):
    depth = pressure.ndim
    below = jnp.concatenate([lower_plane, flow_z[..., :-1, :, :]], axis=depth - 3)
    diverge = flow_x - shifted_behind(flow_x, depth - 2) + (flow_y - shifted_behind(flow_y, depth - 1)) + (flow_z - below)
    fresh = pressure - delta_time * speed_sq * diverge
    return jnp.stack([fresh, flow_x, flow_y, flow_z], axis=depth - 3)

def advance(state, speed_sq, delta_time):
    zero_plane = jnp.zeros_like(state[..., 0, :1, :, :])
    pressure, flow_x, flow_y, flow_z = update_flow(state, zero_plane, delta_time)
    return update_pressure(pressure, flow_x, flow_y, flow_z, zero_plane, speed_sq, delta_time)

def solve_gram(chol, coef):
    lifted = lax.linalg.triangular_solve(chol, coef[..., None], left_side=True, lower=True)
    solved = lax.linalg.triangular_solve(chol, lifted, left_side=True, lower=True, transpose_a=True)
    return solved[..., 0]

def reference(speed, forcing, guess, basis):
    count = guess.shape[0]
    speed_sq = speed * speed
    loads = forcing.reshape(count, 4, forcing.shape[1], forcing.shape[2], forcing.shape[3])

    def fine_step(state, row_index):
        moved = advance(state, speed_sq, DT)
        return moved.at[:, 0].add(loads[:, row_index])

    def sweep(left):
        points = []
        current = left
        for row_index in range(3):
            current = fine_step(current, row_index)
            points.append(current)
        return points

    def from_left(values):
        return jnp.roll(values, 1, axis=0)
    first_points = sweep(from_left(guess))
    relaxed = fine_step(first_points[-1], 3)
    second_points = sweep(from_left(relaxed))
    residue = fine_step(second_points[-1], 3) - relaxed
    flat_basis = basis.reshape(count, basis.shape[1], -1)

    def build(columns):
        moved = columns
        for repeat in range(4):
            moved = advance(moved, speed_sq, DT)
        return (moved - advance(columns, speed_sq, 4 * DT)).reshape(columns.shape[0], -1)
    corrections = lax.map(build, basis)
    gram = jnp.einsum('krn,ksn->krs', flat_basis, flat_basis, precision=exact_mode)
    chol = jnp.linalg.cholesky(gram)

    def candidate(levels):
        left = from_left(levels)
        moved = advance(left, speed_sq, 4 * DT)
        coef = jnp.einsum('krn,kn->kr', flat_basis, left.reshape(count, -1), precision=exact_mode)
        weights = solve_gram(chol, coef)
        extra = jnp.einsum('kr,krn->kn', weights, corrections, precision=exact_mode).reshape(left.shape)
        return moved + extra + residue
    levels = candidate(residue)
    levels = candidate(levels)
    gap = candidate(levels) - levels
    carry = gap[0:4]
    chained = [carry]
    for group in range(1, count // 4):
        carry = advance(advance(carry, speed_sq, 8 * DT), speed_sq, 8 * DT) + gap[4 * group:4 * group + 4]
        chained.append(carry)
    chain = jnp.concatenate(chained, axis=0)
    levels = candidate(levels + chain)
    final_c = relaxed + levels
    third_points = sweep(from_left(final_c))
    states = jnp.stack(third_points + [final_c], axis=1)
    states = states.reshape(count * 4, 4, guess.shape[2], guess.shape[3], guess.shape[4])
    coef = jnp.einsum('krn,kn->kr', flat_basis, final_c.reshape(count, -1), precision=exact_mode)
    coords = solve_gram(chol, coef)
    return (states, coords)
```

```python
import functools

import jax
import jax.numpy as jnp
from jax import lax
from jax.experimental import pallas as pl
from jax.experimental.pallas import tpu as pltpu
from jax.sharding import PartitionSpec as P

DT = 0.045
MESH = pl.DeviceIdType.MESH
F32 = jnp.float32

R1, R2, R3, Y1, Y2, Y3, Y4, X2, X3, X4, GAP, LAST = range(12)
ROUNDS = 12

DEEP = ((0, 5), (0, 5), (1, 5), (0, 3))
THREE = ((0, 5), (0, 5), (2, 4), (1, 2))
TWO = ((1, 5), (0, 3))
ONE = ((2, 4), (1, 2))
OFFSETS = (1, -1, 2, -2)


def kernel(
    n_tm,
    n_space,
    rank,
    speed_hbm,
    forcing_hbm,
    guess_hbm,
    basis_hbm,
    states_ref,
    coords_ref,
    b_ref,
    bt_ref,
    bm_ref,
    guess_ref,
    speed_ref,
    force_ref,
    speed_halo,
    force_halo,
    c2_ref,
    msg_ref,
    halo_ref,
    own_ref,
    yown_ref,
    zout_ref,
    zin_ref,
    rel_ref,
    res_ref,
    x_ref,
    gap_ref,
    fin_ref,
    ar_ref,
    gram_ref,
    inv_ref,
    part_ref,
    w_ref,
    local_sem,
    send_sem,
    recv_sem,
    zsend_sem,
    zrecv_sem,
    start_send,
    start_recv,
    arsend_sem,
    arrecv_sem,
    gsend_sem,
    grecv_sem,
):
    t = lax.axis_index("tm")
    s = lax.axis_index("space")

    def at_t(d):
        return lax.rem(t + (d + n_tm), n_tm)

    def at_s(d):
        return lax.rem(s + (d + n_space), n_space)

    loads = [
        pltpu.make_async_copy(guess_hbm.at[0], guess_ref, local_sem.at[0]),
        pltpu.make_async_copy(speed_hbm, speed_ref, local_sem.at[1]),
        pltpu.make_async_copy(forcing_hbm, force_ref, local_sem.at[2]),
        pltpu.make_async_copy(basis_hbm.at[0], b_ref, local_sem.at[3]),
    ]
    for load in loads:
        load.start()

    def start_row(m, carry):
        c = m // 32
        z = lax.rem(m // 16, 2)
        x = lax.rem(m, 16)
        pltpu.make_async_copy(
            basis_hbm.at[0, :, c, z, x, :], bt_ref.at[c, z, x], local_sem.at[4]
        ).start()
        return carry

    barrier = pltpu.get_barrier_semaphore()
    peers = [(dt, ds) for dt in (1, -1) for ds in (-2, -1, 0, 1, 2)]
    peers += [(4, ds) for ds in (-1, 0, 1)]
    peers += [(0, ds) for ds in range(1, n_space)]
    for dt, ds in peers:
        pl.semaphore_signal(
            barrier, inc=1, device_id=(at_t(dt), at_s(ds)), device_id_type=MESH
        )
    lax.fori_loop(0, 128, start_row, 0)
    pl.semaphore_wait(barrier, len(peers))

    sent = []

    def send(src, dst, ssem, rsem, dt, ds):
        copy = pltpu.make_async_remote_copy(
            src_ref=src,
            dst_ref=dst,
            send_sem=ssem,
            recv_sem=rsem,
            device_id=(at_t(dt), at_s(ds)),
            device_id_type=MESH,
        )
        copy.start()
        sent.append(copy)
        return copy

    plane = guess_ref.shape[2:]
    ix = lax.broadcasted_iota(jnp.int32, plane, 0)
    iy = lax.broadcasted_iota(jnp.int32, plane, 1)
    nx, ny = plane
    zero = jnp.zeros(plane, F32)
    x_low, x_high = ix == 0, ix == nx - 1
    y_low, y_high = iy == 0, iy == ny - 1
    weight = 5.0 - x_low.astype(F32) - y_low.astype(F32)

    def x_ahead(v):
        return jnp.where(x_high, zero, pltpu.roll(v, nx - 1, 0))

    def x_behind(v):
        return jnp.where(x_low, zero, pltpu.roll(v, 1, 0))

    def y_ahead(v):
        return jnp.where(y_high, zero, pltpu.roll(v, ny - 1, 1))

    def y_behind(v):
        return jnp.where(y_low, zero, pltpu.roll(v, 1, 1))

    def flag(cond):
        return jnp.where(cond, 1.0, 0.0).astype(F32)

    e_dn1, e_dn2 = flag(s >= 1), flag(s >= 2)
    e_up1, e_up2 = flag(s <= n_space - 2), flag(s <= n_space - 3)
    floor = {0: e_dn1, -2: e_dn2}

    def lap(p, j):
        below = p[j - 1] - p[j]
        if j in floor:
            below = below * floor[j]
        return (
            (x_ahead(p[j]) + x_behind(p[j]))
            + (y_ahead(p[j]) + y_behind(p[j]))
            + (p[j + 1] - weight * p[j])
            + below
        )

    def c2(j):
        return c2_ref[j + 3]

    def force(n, j):
        if j in (0, 1):
            return force_ref[n, j]
        if j in (-1, -2):
            return force_halo[0, n, j + 2] * e_dn1
        if j in (2, 3):
            return force_halo[1, n, j - 2] * e_up1
        if j == -3:
            return force_halo[2, 0, 1] * e_dn2
        return force_halo[3, 0, 0] * e_up2

    def steps(p, d, h, count, forced=False):
        values, first = [p], None
        for n in range(count):
            depth = count - 1 - n
            planes = range(-depth, 2 + depth)
            laps = {j: lap(p, j) for j in planes}
            if first is None:
                first = laps
            d = {j: d[j] - h * laps[j] for j in planes}
            p = {j: p[j] - (h * c2(j)) * d[j] for j in planes}
            if forced:
                p = {j: p[j] + force(n, j) for j in planes}
            values.append(p)
        return values, first

    def grad(p, j):
        return (x_ahead(p[j]) - p[j], y_ahead(p[j]) - p[j], p[j + 1] - p[j])

    def divergence(state):
        both = []
        for z in range(2):
            both.append(
                (state[1][z] - x_behind(state[1][z]))
                + (state[2][z] - y_behind(state[2][z]))
            )
        return both[0] + state[3][0], both[1] + (state[3][1] - state[3][0])

    def load_state(ref):
        return [[ref[c, z] for z in range(2)] for c in range(4)]

    def store_state(ref, state):
        for c in range(4):
            for z in range(2):
                ref[c, z] = state[c][z]

    def combine(fn, *states):
        return [[fn(*[u[c][z] for u in states]) for z in range(2)] for c in range(4)]

    def write_msg(ref, state, deep=True):
        if deep:
            low, high = divergence(state)
            ref[0] = low
            ref[4] = high
        ref[1] = state[0][0]
        ref[2] = state[0][1]
        ref[3] = state[3][1]

    def unpack(halo, own_p, own_d, own_vz, depth):
        p = {0: own_p[0], 1: own_p[1]}
        vz_below = halo[0, 3] * e_dn1
        p[-1] = halo[0, 2] * e_dn1
        p[2] = halo[1, 1] * e_up1
        d = {0: own_d[0] - vz_below, 1: own_d[1]}
        if depth >= 2:
            p[-2] = halo[0, 1] * e_dn1
            p[3] = halo[1, 2] * e_up1
            d[-1] = halo[0, 4]
            d[2] = halo[1, 0] - own_vz
        if depth >= 3:
            p[-3] = halo[2, 2] * e_dn2
            p[4] = halo[3, 1] * e_up2
            d[-2] = halo[0, 0] - halo[2, 3] * e_dn2
            d[3] = halo[1, 4]
        if depth >= 4:
            p[-4] = halo[2, 1] * e_dn2
            p[5] = halo[3, 2] * e_up2
            d[-3] = halo[2, 4]
            d[4] = halo[3, 0] - halo[1, 3]
        return p, d

    def send_halo(i, slices, dt):
        for k, (low, high) in enumerate(slices):
            part = pl.ds(low, high - low)
            send(
                msg_ref.at[i, part],
                halo_ref.at[i, k, part],
                send_sem.at[i, k],
                recv_sem.at[i, k],
                dt,
                OFFSETS[k],
            )

    def wait_halo(i, slices, dt):
        for k, (low, high) in enumerate(slices):
            part = pl.ds(low, high - low)
            pltpu.make_async_remote_copy(
                src_ref=msg_ref.at[i, part],
                dst_ref=halo_ref.at[i, k, part],
                send_sem=send_sem.at[i, k],
                recv_sem=recv_sem.at[i, k],
                device_id=(at_t(dt), at_s(OFFSETS[k])),
                device_id_type=MESH,
            ).wait_recv()

    def send_own(i, src, dst, dt):
        return send(src, dst, send_sem.at[i, 4], recv_sem.at[i, 4], dt, 0)

    def send_state(i, ref, dt):
        return send_own(i, ref, own_ref.at[i], dt)

    def halo_of(i):
        return halo_ref.at[i]

    rows = lax.broadcasted_iota(jnp.int32, (rank, 128), 0)
    lanes = lax.broadcasted_iota(jnp.int32, (rank, 128), 1)
    diagonal = rows == lanes

    def to_row(column):
        spread = jnp.where(diagonal, jnp.broadcast_to(column, (rank, 128)), 0.0)
        return jnp.sum(spread, axis=0, keepdims=True)

    def share_products(i, state_ref):
        def group(g, carry):
            out = []
            for k in range(8):
                total = jnp.zeros((8, 128), F32)
                for c in range(4):
                    for z in range(2):
                        for half in range(nx // 8):
                            part = slice(half * 8, half * 8 + 8)
                            total = total + (
                                b_ref[g * 8 + k, c, z, part, :] * state_ref[c, z, part, :]
                            )
                out.append(jnp.sum(total, axis=0, keepdims=True))
            part_ref[pl.ds(pl.multiple_of(g * 8, 8), 8), :] = jnp.concatenate(out, axis=0)
            return carry

        lax.fori_loop(0, rank // 8, group, 0)
        ar_ref[i, s] = to_row(jnp.sum(part_ref[...], axis=1, keepdims=True))
        for j in range(1, n_space):
            send(
                ar_ref.at[i, s],
                ar_ref.at[i, s],
                arsend_sem.at[i, j],
                arrecv_sem.at[i, j],
                0,
                j,
            )

    def solved(i):
        for j in range(1, n_space):
            pltpu.make_async_remote_copy(
                src_ref=ar_ref.at[i, s],
                dst_ref=ar_ref.at[i, at_s(-j)],
                send_sem=arsend_sem.at[i, j],
                recv_sem=arrecv_sem.at[i, j],
                device_id=(t, at_s(j)),
                device_id_type=MESH,
            ).wait_recv()
        total = ar_ref[i, 0]
        for j in range(1, n_space):
            total = total + ar_ref[i, j]
        moved = pltpu.roll(jnp.broadcast_to(total, (8, 128)), rank, 1)[0:1]
        product = jnp.where(lanes >= rank, inv_ref[...] * moved, 0.0)
        return jnp.sum(product, axis=1, keepdims=True)

    def combine_columns(i, weights):
        w_ref[...] = jnp.broadcast_to(weights, (rank, 128))

        def group(g, acc):
            for k in range(4):
                r = g * 4 + k
                w = jnp.broadcast_to(w_ref[pl.ds(r, 1), :], plane)
                acc = tuple(acc[m] + w * bm_ref[r, m] for m in range(5))
            return acc

        acc = lax.fori_loop(0, rank // 4, group, (zero,) * 5)
        for m in range(5):
            msg_ref[i, m] = acc[m]

    def eliminate(low, high):
        def step(k, carry):
            m = inv_ref[...]
            row = inv_ref[pl.ds(k, 1), :]
            col = jnp.sum(jnp.where(lanes == k, m, 0.0), axis=1, keepdims=True)
            pivot = jnp.sum(jnp.where(lanes[0:1] == k, row, 0.0), axis=1, keepdims=True)
            row = row / pivot
            inv_ref[...] = jnp.where(rows == k, row, m - col * row)
            return carry

        lax.fori_loop(low, high, step, 0)

    loads[0].wait()
    write_msg(msg_ref.at[R1], load_state(guess_ref))
    send_halo(R1, DEEP, 1)
    send_state(R1, guess_ref, 1)
    loads[1].wait()
    loads[2].wait()
    edge = (None, None, pl.ds(1, 1), pl.ds(0, 1))
    starts = []
    for k in range(4):
        if edge[k] is None:
            pair = [
                (speed_ref, speed_halo.at[k]),
                (force_ref.at[pl.ds(0, 3)], force_halo.at[k]),
            ]
        else:
            pair = [
                (speed_ref.at[edge[k]], speed_halo.at[k, edge[k]]),
                (
                    force_ref.at[pl.ds(0, 1), edge[k]],
                    force_halo.at[k, pl.ds(0, 1), edge[k]],
                ),
            ]
        for m, (src, dst) in enumerate(pair):
            starts.append(
                send(src, dst, start_send.at[k, m], start_recv.at[k, m], 0, OFFSETS[k])
            )

    loads[3].wait()

    def column_msg(r, carry):
        state = [[b_ref[r, c, z] for z in range(2)] for c in range(4)]
        write_msg(bm_ref.at[r], state)
        return carry

    lax.fori_loop(0, rank, column_msg, 0)
    pltpu.make_async_copy(bt_ref, bt_ref, local_sem.at[4]).wait()

    def gram_part(i, acc):
        c = i // 4
        z = lax.rem(i // 2, 2)
        x = lax.rem(i, 2) * 8
        flat = jnp.concatenate([bt_ref[c, z, x + k] for k in range(8)], axis=1)
        return acc + lax.dot_general(
            flat,
            flat,
            (((1,), (1,)), ((), ())),
            precision=lax.Precision.HIGHEST,
            preferred_element_type=F32,
        )

    gram = lax.fori_loop(0, 16, gram_part, jnp.zeros((rank, rank), F32))
    half = rank // 2
    gram_ref[s] = jnp.concatenate([gram[:half], gram[half:]], axis=1)
    for j in range(1, n_space):
        send(gram_ref.at[s], gram_ref.at[s], gsend_sem.at[j], grecv_sem.at[j], 0, j)

    for copy in starts:
        copy.wait_recv()
    for j, value, on in (
        (0, speed_ref[0], None),
        (1, speed_ref[1], None),
        (-1, speed_halo[0, 1], e_dn1),
        (-2, speed_halo[0, 0], e_dn1),
        (2, speed_halo[1, 0], e_up1),
        (3, speed_halo[1, 1], e_up1),
        (-3, speed_halo[2, 1], e_dn2),
        (4, speed_halo[3, 0], e_up2),
    ):
        squared = value * value
        c2_ref[j + 3] = squared if on is None else squared * on

    def four_forced(i):
        wait_halo(i, DEEP, 1)
        state = load_state(own_ref.at[i])
        low, high = divergence(state)
        p, d = unpack(halo_of(i), state[0], (low, high), state[3][1], 4)
        values, _ = steps(p, d, DT, 4, forced=True)
        total = {
            j: (values[0][j] + values[1][j]) + (values[2][j] + values[3][j])
            for j in range(0, 3)
        }
        out = [[values[4][0], values[4][1]], [None] * 2, [None] * 2, [None] * 2]
        for z in range(2):
            for c, slope in enumerate(grad(total, z)):
                out[c + 1][z] = state[c + 1][z] - DT * slope
        return out

    def wait_state(i, dt):
        pltpu.make_async_remote_copy(
            src_ref=own_ref.at[i],
            dst_ref=own_ref.at[i],
            send_sem=send_sem.at[i, 4],
            recv_sem=recv_sem.at[i, 4],
            device_id=(at_t(dt), s),
            device_id_type=MESH,
        ).wait_recv()

    wait_state(R1, 1)
    relaxed = four_forced(R1)
    store_state(rel_ref, relaxed)
    write_msg(msg_ref.at[R2], relaxed)
    send_halo(R2, DEEP, 1)
    send_state(R2, rel_ref, 1)

    for j in range(1, n_space):
        pltpu.make_async_remote_copy(
            src_ref=gram_ref.at[s],
            dst_ref=gram_ref.at[at_s(-j)],
            send_sem=gsend_sem.at[j],
            recv_sem=grecv_sem.at[j],
            device_id=(t, at_s(j)),
            device_id_type=MESH,
        ).wait_recv()
    whole = gram_ref[0]
    for j in range(1, n_space):
        whole = whole + gram_ref[j]
    unit = (lanes == rows + rank).astype(F32)
    left = lanes[:half] < rank
    inv_ref[0:half, :] = jnp.where(left, whole, unit[:half])
    inv_ref[half:rank, :] = jnp.where(left, pltpu.roll(whole, 128 - rank, 1), unit[half:])
    eliminate(0, 24)

    wait_state(R2, 1)
    residue = combine(lambda a, b: a - b, four_forced(R2), load_state(rel_ref))
    store_state(res_ref, residue)
    write_msg(msg_ref.at[R3], residue, deep=False)
    send_state(R3, res_ref, 1)
    send_halo(R3, ONE, 1)
    eliminate(24, 40)

    def coarse(state, halo):
        p, d = unpack(halo, state[0], divergence(state), None, 1)
        values, _ = steps(p, d, 4 * DT, 1)
        out = [[values[1][0], values[1][1]], [None] * 2, [None] * 2, [None] * 2]
        for z in range(2):
            for c, slope in enumerate(grad(p, z)):
                out[c + 1][z] = state[c + 1][z] - (4 * DT) * slope
        return out

    def correction(halo, own):
        p, d = unpack(halo, (own[1], own[2]), (own[0], own[4]), own[3], 4)
        values, first = steps(p, d, DT, 4)
        out = [[None] * 2 for _ in range(4)]
        for z in range(2):
            slow = p[z] - (4 * DT * c2(z)) * (d[z] - (4 * DT) * first[z])
            out[0][z] = values[4][z] - slow
        total = {
            j: (values[1][j] - p[j]) + (values[2][j] - p[j]) + (values[3][j] - p[j])
            for j in range(0, 3)
        }
        for z in range(2):
            for c, slope in enumerate(grad(total, z)):
                out[c + 1][z] = -DT * slope
        return out

    def add(a, b):
        return a + b

    def candidate(n, i_y, i_x, x_state_ref, last):
        share_products(n, x_state_ref)
        wait_halo(i_x, ONE, 1 if i_x == R3 else 0)
        z = combine(add, coarse(load_state(x_state_ref), halo_of(i_x)), load_state(res_ref))
        store_state(zout_ref.at[n], z)
        if not last:
            send(zout_ref.at[n], zin_ref.at[n], zsend_sem.at[n], zrecv_sem.at[n], 1, 0)
        if n == 0:
            eliminate(40, rank)
        combine_columns(i_y, solved(n))
        dt = 0 if last else 1
        send_halo(i_y, DEEP, dt)
        if last:
            wait_halo(i_y, DEEP, dt)
            return combine(
                add,
                load_state(zout_ref.at[n]),
                correction(halo_of(i_y), msg_ref.at[i_y]),
            )
        own = send_own(i_y, msg_ref.at[i_y], yown_ref.at[n], dt)
        pltpu.make_async_remote_copy(
            src_ref=zout_ref.at[n],
            dst_ref=zin_ref.at[n],
            send_sem=zsend_sem.at[n],
            recv_sem=zrecv_sem.at[n],
            device_id=(at_t(1), s),
            device_id_type=MESH,
        ).wait_recv()
        own.wait_recv()
        wait_halo(i_y, DEEP, dt)
        return combine(
            add, load_state(zin_ref.at[n]), correction(halo_of(i_y), yown_ref.at[n])
        )

    def announce(i, ref, state):
        store_state(ref, state)
        write_msg(msg_ref.at[i], state, deep=False)
        send_halo(i, ONE, 0)

    wait_state(R3, 1)
    announce(X2, x_ref.at[0], candidate(0, Y1, R3, own_ref.at[R3], False))
    announce(X3, x_ref.at[1], candidate(1, Y2, X2, x_ref.at[0], False))
    third = candidate(2, Y3, X3, x_ref.at[1], False)
    store_state(x_ref.at[2], third)

    gap = combine(lambda a, b: a - b, third, load_state(x_ref.at[1]))
    store_state(gap_ref, gap)
    write_msg(msg_ref.at[GAP], gap)
    send_halo(GAP, TWO, 4)
    send_state(GAP, gap_ref, 4)
    wait_halo(GAP, TWO, 4)
    wait_state(GAP, 4)
    state = load_state(own_ref.at[GAP])
    p, d = unpack(halo_of(GAP), state[0], divergence(state), state[3][1], 2)
    values, _ = steps(p, d, 8 * DT, 2)
    total = {j: values[0][j] + values[1][j] for j in range(0, 3)}
    behind = [[values[2][0], values[2][1]], [None] * 2, [None] * 2, [None] * 2]
    for z in range(2):
        for c, slope in enumerate(grad(total, z)):
            behind[c + 1][z] = state[c + 1][z] - (8 * DT) * slope
    late = flag(lax.rem(t + (n_tm - 1), n_tm) >= 4)
    announce(
        X4,
        x_ref.at[3],
        combine(lambda a, b: a + late * b, load_state(x_ref.at[2]), behind),
    )
    levels = candidate(3, Y4, X4, x_ref.at[3], True)

    final = combine(add, load_state(rel_ref), levels)
    store_state(fin_ref, final)
    write_msg(msg_ref.at[LAST], final)
    send_halo(LAST, THREE, 1)
    send_state(LAST, fin_ref, 1)
    share_products(4, fin_ref)
    store_state(states_ref.at[3], final)
    wait_state(LAST, 1)
    wait_halo(LAST, THREE, 1)
    state = load_state(own_ref.at[LAST])
    p, d = unpack(halo_of(LAST), state[0], divergence(state), state[3][1], 3)
    values, _ = steps(p, d, DT, 3, forced=True)
    for n in range(3):
        for z in range(2):
            state[0][z] = values[n + 1][z]
            for c, slope in enumerate(grad(values[n], z)):
                state[c + 1][z] = state[c + 1][z] - DT * slope
        store_state(states_ref.at[n], state)
    coords_ref[...] = to_row(solved(4))[:, :rank]

    for copy in sent:
        copy.wait_send()


def body(n_tm, n_space, speed, forcing, guess, basis):
    rank = basis.shape[1]
    plane = speed.shape[1:]
    vmem = functools.partial(pltpu.VMEM, dtype=F32)
    dma = pltpu.SemaphoreType.DMA
    state = (4, 2, *plane)
    msg = (5, *plane)
    scratch = [
        vmem((rank, *state)),
        vmem((4, 2, plane[0], rank, plane[1])),
        vmem((rank, *msg)),
        vmem(state),
        vmem((2, *plane)),
        vmem((4, 2, *plane)),
        vmem((4, 2, *plane)),
        vmem((4, 3, 2, *plane)),
        vmem((8, *plane)),
        vmem((ROUNDS, *msg)),
        vmem((ROUNDS, 4, *msg)),
        vmem((ROUNDS, *state)),
        vmem((3, *msg)),
        vmem((4, *state)),
        vmem((3, *state)),
        vmem(state),
        vmem(state),
        vmem((4, *state)),
        vmem(state),
        vmem(state),
        vmem((5, n_space, 1, 128)),
        vmem((n_space, rank // 2, 128)),
        vmem((rank, 128)),
        vmem((rank, 128)),
        vmem((rank, 128)),
        dma((5,)),
        dma((ROUNDS, 5)),
        dma((ROUNDS, 5)),
        dma((3,)),
        dma((3,)),
        dma((4, 2)),
        dma((4, 2)),
        dma((5, n_space)),
        dma((5, n_space)),
        dma((n_space,)),
        dma((n_space,)),
    ]
    return pl.pallas_call(
        functools.partial(kernel, n_tm, n_space, rank),
        out_shape=(
            jax.ShapeDtypeStruct((4, *state), F32),
            jax.ShapeDtypeStruct((1, rank), F32),
        ),
        in_specs=[pl.BlockSpec(memory_space=pl.ANY)] * 4,
        out_specs=(
            pl.BlockSpec(memory_space=pltpu.VMEM),
            pl.BlockSpec(memory_space=pltpu.VMEM),
        ),
        scratch_shapes=scratch,
        compiler_params=pltpu.CompilerParams(collective_id=0, has_side_effects=True),
    )(speed, forcing, guess, basis)


def solution(mesh):
    placed = (
        P("space", None, None),
        P("tm", "space", None, None),
        P("tm", None, "space", None, None),
        P("tm", None, None, "space", None, None),
    )
    return jax.shard_map(
        functools.partial(body, mesh.shape["tm"], mesh.shape["space"]),
        mesh=mesh,
        in_specs=placed,
        out_specs=(P("tm", None, "space", None, None), P("tm", None)),
        check_vma=False,
    )
```

```python
import functools
import math

import jax
import jax.numpy as jnp
from jax import lax
from jax.experimental import pallas as pl
from jax.experimental.pallas import tpu as pltpu
from jax.sharding import PartitionSpec as P

DT = 0.045
MESH = pl.DeviceIdType.MESH
F32 = jnp.float32

R1, R2, R3, Y1, Y2, Y3, Y4, X2, X3, X4, GAP, LAST = range(12)
ROUNDS = 12

DEEP = ((0, 5), (0, 5), (1, 5), (0, 3))
THREE = ((0, 5), (0, 5), (2, 4), (1, 2))
TWO = ((1, 5), (0, 3))
ONE = ((2, 4), (1, 2))
OFFSETS = (1, -1, 2, -2)


def kernel(
    n_tm,
    n_space,
    rank,
    speed_hbm,
    forcing_hbm,
    guess_hbm,
    basis_hbm,
    states_ref,
    coords_ref,
    b_ref,
    bt_ref,
    bm_ref,
    guess_ref,
    speed_ref,
    force_ref,
    speed_halo,
    force_halo,
    c2_ref,
    msg_ref,
    halo_ref,
    own_ref,
    yown_ref,
    zout_ref,
    zin_ref,
    rel_ref,
    res_ref,
    x_ref,
    gap_ref,
    fin_ref,
    ar_ref,
    gram_ref,
    inv_ref,
    part_ref,
    w_ref,
    local_sem,
    send_sem,
    gap_sem,
    recv_sem,
    ar_send_sem,
    ar_sem,
    gram_sem,
):
    plane = guess_ref.shape[2:]
    t = lax.axis_index("tm")
    s = lax.axis_index("space")

    def at_t(d):
        return lax.rem(t + (d + n_tm), n_tm)

    def at_s(d):
        return lax.rem(s + (d + n_space), n_space)

    loads = [
        pltpu.make_async_copy(guess_hbm.at[0], guess_ref, local_sem.at[0]),
        pltpu.make_async_copy(speed_hbm, speed_ref, local_sem.at[1]),
        pltpu.make_async_copy(forcing_hbm, force_ref, local_sem.at[2]),
        pltpu.make_async_copy(basis_hbm.at[0], b_ref, local_sem.at[3]),
    ]
    for load in loads:
        load.start()

    def start_rows(m, carry):
        c = m // 2
        z = lax.rem(m, 2)
        for x in range(plane[0]):
            pltpu.make_async_copy(
                basis_hbm.at[0, :, c, z, x, :], bt_ref.at[c, z, x], local_sem.at[4]
            ).start()
        return carry

    barrier = pltpu.get_barrier_semaphore()
    peers = [(dt, ds) for dt in (1, -1) for ds in (-2, -1, 0, 1, 2)]
    peers += [(4, ds) for ds in (-1, 0, 1)]
    peers += [(0, ds) for ds in range(1, n_space)]
    with jax.named_scope("signals"):
        for dt, ds in peers:
            pl.semaphore_signal(
                barrier, inc=1, device_id=(at_t(dt), at_s(ds)), device_id_type=MESH
            )
    with jax.named_scope("rows"):
        lax.fori_loop(0, 8, start_rows, 0)

    sent = []

    def words(ref):
        return math.prod(ref.shape)

    def send(src, dst, rsem, dt, ds, ssem=None):
        pltpu.make_async_remote_copy(
            src_ref=src,
            dst_ref=dst,
            send_sem=send_sem.at[0] if ssem is None else ssem,
            recv_sem=rsem,
            device_id=(at_t(dt), at_s(ds)),
            device_id_type=MESH,
        ).start()
        if ssem is None:
            sent.append(words(src))

    def wait_planes(sem, planes):
        part = bm_ref.reshape(rank * 5, *plane).at[pl.ds(0, planes)]
        pltpu.make_async_copy(part, part, sem).wait()

    ix = lax.broadcasted_iota(jnp.int32, plane, 0)
    iy = lax.broadcasted_iota(jnp.int32, plane, 1)
    nx, ny = plane
    zero = jnp.zeros(plane, F32)
    x_low, x_high = ix == 0, ix == nx - 1
    y_low, y_high = iy == 0, iy == ny - 1
    weight = 5.0 - x_low.astype(F32) - y_low.astype(F32)

    def x_ahead(v):
        return jnp.where(x_high, zero, pltpu.roll(v, nx - 1, 0))

    def x_behind(v):
        return jnp.where(x_low, zero, pltpu.roll(v, 1, 0))

    def y_ahead(v):
        return jnp.where(y_high, zero, pltpu.roll(v, ny - 1, 1))

    def y_behind(v):
        return jnp.where(y_low, zero, pltpu.roll(v, 1, 1))

    def flag(cond):
        return jnp.where(cond, 1.0, 0.0).astype(F32)

    e_dn1, e_dn2 = flag(s >= 1), flag(s >= 2)
    e_up1, e_up2 = flag(s <= n_space - 2), flag(s <= n_space - 3)
    floor = {0: e_dn1, -2: e_dn2}

    def lap(p, j):
        below = p[j - 1] - p[j]
        if j in floor:
            below = below * floor[j]
        return (
            (x_ahead(p[j]) + x_behind(p[j]))
            + (y_ahead(p[j]) + y_behind(p[j]))
            + (p[j + 1] - weight * p[j])
            + below
        )

    def c2(j):
        return c2_ref[j + 3]

    def force(n, j):
        if j in (0, 1):
            return force_ref[n, j]
        if j in (-1, -2):
            return force_halo[0, n, j + 2] * e_dn1
        if j in (2, 3):
            return force_halo[1, n, j - 2] * e_up1
        if j == -3:
            return force_halo[2, 0, 1] * e_dn2
        return force_halo[3, 0, 0] * e_up2

    def steps(p, d, h, count, forced=False):
        values, first = [p], None
        for n in range(count):
            depth = count - 1 - n
            planes = range(-depth, 2 + depth)
            laps = {j: lap(p, j) for j in planes}
            if first is None:
                first = laps
            d = {j: d[j] - h * laps[j] for j in planes}
            p = {j: p[j] - (h * c2(j)) * d[j] for j in planes}
            if forced:
                p = {j: p[j] + force(n, j) for j in planes}
            values.append(p)
        return values, first

    def grad(p, j):
        return (x_ahead(p[j]) - p[j], y_ahead(p[j]) - p[j], p[j + 1] - p[j])

    def divergence(state):
        both = []
        for z in range(2):
            both.append(
                (state[1][z] - x_behind(state[1][z]))
                + (state[2][z] - y_behind(state[2][z]))
            )
        return both[0] + state[3][0], both[1] + (state[3][1] - state[3][0])

    def load_state(ref):
        return [[ref[c, z] for z in range(2)] for c in range(4)]

    def store_state(ref, state):
        for c in range(4):
            for z in range(2):
                ref[c, z] = state[c][z]

    def combine(fn, *states):
        return [[fn(*[u[c][z] for u in states]) for z in range(2)] for c in range(4)]

    def write_msg(ref, state, deep=True):
        if deep:
            low, high = divergence(state)
            ref[0] = low
            ref[4] = high
        ref[1] = state[0][0]
        ref[2] = state[0][1]
        ref[3] = state[3][1]

    def unpack(halo, own_p, own_d, own_vz, depth):
        p = {0: own_p[0], 1: own_p[1]}
        vz_below = halo[0, 3] * e_dn1
        p[-1] = halo[0, 2] * e_dn1
        p[2] = halo[1, 1] * e_up1
        d = {0: own_d[0] - vz_below, 1: own_d[1]}
        if depth >= 2:
            p[-2] = halo[0, 1] * e_dn1
            p[3] = halo[1, 2] * e_up1
            d[-1] = halo[0, 4]
            d[2] = halo[1, 0] - own_vz
        if depth >= 3:
            p[-3] = halo[2, 2] * e_dn2
            p[4] = halo[3, 1] * e_up2
            d[-2] = halo[0, 0] - halo[2, 3] * e_dn2
            d[3] = halo[1, 4]
        if depth >= 4:
            p[-4] = halo[2, 1] * e_dn2
            p[5] = halo[3, 2] * e_up2
            d[-3] = halo[2, 4]
            d[4] = halo[3, 0] - halo[1, 3]
        return p, d

    def send_halo(i, slices, dt, ssem=None):
        for k in reversed(range(len(slices))):
            low, high = slices[k]
            part = pl.ds(low, high - low)
            send(
                msg_ref.at[i, part],
                halo_ref.at[i, k, part],
                recv_sem.at[i],
                dt,
                OFFSETS[k],
                ssem,
            )

    def planes_of(slices):
        return sum(high - low for low, high in slices)

    def send_own(i, src, dst, dt, ssem=None):
        send(src, dst, recv_sem.at[i], dt, 0, ssem)

    def send_state(i, ref, dt, ssem=None):
        send_own(i, ref, own_ref.at[i], dt, ssem)

    def wait_round(i, slices, more):
        with jax.named_scope(f"wait_round{i}"):
            wait_planes(recv_sem.at[i], planes_of(slices) + more)

    def halo_of(i):
        return halo_ref.at[i]

    rows = lax.broadcasted_iota(jnp.int32, (rank, 128), 0)
    lanes = lax.broadcasted_iota(jnp.int32, (rank, 128), 1)
    diagonal = rows == lanes

    far_first = sorted(range(1, n_space), key=lambda j: abs(abs(j - n_space // 2) - 2))

    def to_row(column):
        spread = jnp.where(diagonal, jnp.broadcast_to(column, (rank, 128)), 0.0)
        return jnp.sum(spread, axis=0, keepdims=True)

    def share_products(i, state_ref):
        def group(g, carry):
            out = []
            for k in range(16):
                total = jnp.zeros((8, 128), F32)
                for c in range(4):
                    for z in range(2):
                        for half in range(nx // 8):
                            part = slice(half * 8, half * 8 + 8)
                            total = total + (
                                b_ref[g * 16 + k, c, z, part, :] * state_ref[c, z, part, :]
                            )
                out.append(jnp.sum(total, axis=0, keepdims=True))
            part_ref[pl.ds(pl.multiple_of(g * 16, 16), 16), :] = jnp.concatenate(out, axis=0)
            return carry

        with jax.named_scope(f"products{i}"):
            lax.fori_loop(0, rank // 16, group, 0)
            ar_ref[i, s] = to_row(jnp.sum(part_ref[...], axis=1, keepdims=True))
            for j in far_first:
                send(ar_ref.at[i, s], ar_ref.at[i, s], ar_sem.at[i], 0, j, ar_send_sem.at[i])

    def solved(i):
        with jax.named_scope(f"wait_ar{i}"):
            part = ar_ref.at[i, pl.ds(0, n_space - 1)]
            pltpu.make_async_copy(part, part, ar_sem.at[i]).wait()
        total = ar_ref[i, 0]
        for j in range(1, n_space):
            total = total + ar_ref[i, j]
        moved = pltpu.roll(jnp.broadcast_to(total, (8, 128)), rank, 1)[0:1]
        product = jnp.where(lanes >= rank, inv_ref[...] * moved, 0.0)
        return jnp.sum(product, axis=1, keepdims=True)

    def combine_columns(i, weights):
        w_ref[...] = jnp.broadcast_to(weights, (rank, 128))

        def group(g, acc):
            for k in range(4):
                r = g * 4 + k
                w = jnp.broadcast_to(w_ref[pl.ds(r, 1), :], plane)
                acc = tuple(acc[m] + w * bm_ref[r, m] for m in range(5))
            return acc

        with jax.named_scope(f"columns{i}"):
            acc = lax.fori_loop(0, rank // 4, group, (zero,) * 5)
            for m in range(5):
                msg_ref[i, m] = acc[m]

    def eliminate(low, high):
        def step(k, carry):
            m = inv_ref[...]
            row = inv_ref[pl.ds(k, 1), :]
            col = jnp.sum(jnp.where(lanes == k, m, 0.0), axis=1, keepdims=True)
            pivot = jnp.sum(jnp.where(lanes[0:1] == k, row, 0.0), axis=1, keepdims=True)
            row = row / pivot
            inv_ref[...] = jnp.where(rows == k, row, m - col * row)
            return carry

        with jax.named_scope(f"eliminate{low}"):
            lax.fori_loop(low, high, step, 0)

    def wait_rows():
        with jax.named_scope("wait_bt"):
            pltpu.make_async_copy(bt_ref, bt_ref, local_sem.at[4]).wait()

    def gram_part(i, acc):
        c = i // 4
        z = lax.rem(i // 2, 2)
        x = lax.rem(i, 2) * 8
        flat = jnp.concatenate([bt_ref[c, z, x + k] for k in range(8)], axis=1)
        high = flat.astype(jnp.bfloat16)
        rest = flat - high.astype(F32)
        middle = rest.astype(jnp.bfloat16)
        low = (rest - middle.astype(F32)).astype(jnp.bfloat16)
        stacked = jnp.concatenate([high, middle, low], axis=0)
        return acc + lax.dot_general(
            stacked,
            stacked,
            (((1,), (1,)), ((), ())),
            preferred_element_type=F32,
        )

    def send_gram():
        with jax.named_scope("gram"):
            acc = lax.fori_loop(0, 16, gram_part, jnp.zeros((3 * rank, 3 * rank), F32))
        acc = acc[2 * rank :] + acc[rank : 2 * rank] + acc[:rank]
        gram = acc[:, 2 * rank :] + acc[:, rank : 2 * rank] + acc[:, :rank]
        half = rank // 2
        gram_ref[s] = jnp.concatenate([gram[:half], gram[half:]], axis=1)
        for j in far_first:
            send(gram_ref.at[s], gram_ref.at[s], gram_sem.at[0], 0, j)

    with jax.named_scope("wait_basis"):
        loads[3].wait()

    def column_msg(g, carry):
        for k in range(8):
            write_msg(bm_ref.at[g * 8 + k], load_state(b_ref.at[g * 8 + k]))
        return carry

    with jax.named_scope("column_msg"):
        lax.fori_loop(0, rank // 8, column_msg, 0)
    with jax.named_scope("barrier"):
        pl.semaphore_wait(barrier, len(peers))

    with jax.named_scope("wait_guess"):
        loads[0].wait()
    write_msg(msg_ref.at[R1], load_state(guess_ref))
    send_halo(R1, DEEP, 1)
    send_state(R1, guess_ref, 1)
    with jax.named_scope("wait_load12"):
        loads[1].wait()
        loads[2].wait()
    edge = (None, None, pl.ds(1, 1), pl.ds(0, 1))
    for k in (3, 2, 1, 0):
        if edge[k] is None:
            pair = [
                (speed_ref, speed_halo.at[k]),
                (force_ref.at[pl.ds(0, 3)], force_halo.at[k]),
            ]
        else:
            pair = [
                (speed_ref.at[edge[k]], speed_halo.at[k, edge[k]]),
                (
                    force_ref.at[pl.ds(0, 1), edge[k]],
                    force_halo.at[k, pl.ds(0, 1), edge[k]],
                ),
            ]
        for src, dst in pair:
            send(src, dst, recv_sem.at[R1], 0, OFFSETS[k])

    wait_rows()
    send_gram()

    wait_round(R1, DEEP, 8 + 6 + 14)
    for j, value, on in (
        (0, speed_ref[0], None),
        (1, speed_ref[1], None),
        (-1, speed_halo[0, 1], e_dn1),
        (-2, speed_halo[0, 0], e_dn1),
        (2, speed_halo[1, 0], e_up1),
        (3, speed_halo[1, 1], e_up1),
        (-3, speed_halo[2, 1], e_dn2),
        (4, speed_halo[3, 0], e_up2),
    ):
        squared = value * value
        c2_ref[j + 3] = squared if on is None else squared * on

    def four_forced(i):
        state = load_state(own_ref.at[i])
        low, high = divergence(state)
        p, d = unpack(halo_of(i), state[0], (low, high), state[3][1], 4)
        values, _ = steps(p, d, DT, 4, forced=True)
        total = {
            j: (values[0][j] + values[1][j]) + (values[2][j] + values[3][j])
            for j in range(0, 3)
        }
        out = [[values[4][0], values[4][1]], [None] * 2, [None] * 2, [None] * 2]
        for z in range(2):
            for c, slope in enumerate(grad(total, z)):
                out[c + 1][z] = state[c + 1][z] - DT * slope
        return out

    relaxed = four_forced(R1)
    store_state(rel_ref, relaxed)
    write_msg(msg_ref.at[R2], relaxed)
    send_halo(R2, DEEP, 1)
    send_state(R2, rel_ref, 1)

    wait_round(R2, DEEP, 8)
    residue = combine(lambda a, b: a - b, four_forced(R2), load_state(rel_ref))
    store_state(res_ref, residue)
    write_msg(msg_ref.at[R3], residue, deep=False)
    send_state(R3, res_ref, 1)
    send_halo(R3, ONE, 1)

    with jax.named_scope("wait_gram"):
        part = gram_ref.at[pl.ds(0, n_space - 1)]
        pltpu.make_async_copy(part, part, gram_sem.at[0]).wait()
    whole = gram_ref[0]
    for j in range(1, n_space):
        whole = whole + gram_ref[j]
    half = rank // 2
    unit = (lanes == rows + rank).astype(F32)
    left = lanes[:half] < rank
    inv_ref[0:half, :] = jnp.where(left, whole, unit[:half])
    inv_ref[half:rank, :] = jnp.where(left, pltpu.roll(whole, 128 - rank, 1), unit[half:])
    eliminate(0, 24)


    def coarse(state, halo):
        p, d = unpack(halo, state[0], divergence(state), None, 1)
        values, _ = steps(p, d, 4 * DT, 1)
        out = [[values[1][0], values[1][1]], [None] * 2, [None] * 2, [None] * 2]
        for z in range(2):
            for c, slope in enumerate(grad(p, z)):
                out[c + 1][z] = state[c + 1][z] - (4 * DT) * slope
        return out

    def correction(halo, own):
        p, d = unpack(halo, (own[1], own[2]), (own[0], own[4]), own[3], 4)
        values, first = steps(p, d, DT, 4)
        out = [[None] * 2 for _ in range(4)]
        for z in range(2):
            slow = p[z] - (4 * DT * c2(z)) * (d[z] - (4 * DT) * first[z])
            out[0][z] = values[4][z] - slow
        total = {
            j: (values[1][j] - p[j]) + (values[2][j] - p[j]) + (values[3][j] - p[j])
            for j in range(0, 3)
        }
        for z in range(2):
            for c, slope in enumerate(grad(total, z)):
                out[c + 1][z] = -DT * slope
        return out

    def add(a, b):
        return a + b

    def candidate(n, i_y, i_x, x_state_ref, last):
        share_products(n, x_state_ref)
        if i_x != R3:
            wait_round(i_x, ONE, 0)
        z = combine(add, coarse(load_state(x_state_ref), halo_of(i_x)), load_state(res_ref))
        store_state(zout_ref.at[n], z)
        if not last:
            send(zout_ref.at[n], zin_ref.at[n], recv_sem.at[i_y], 1, 0)
        if n == 0:
            eliminate(24, rank)
        combine_columns(i_y, solved(n))
        dt = 0 if last else 1
        send_halo(i_y, DEEP, dt)
        if last:
            wait_round(i_y, DEEP, 0)
            return combine(
                add,
                load_state(zout_ref.at[n]),
                correction(halo_of(i_y), msg_ref.at[i_y]),
            )
        send_own(i_y, msg_ref.at[i_y], yown_ref.at[n], dt)
        wait_round(i_y, DEEP, 5 + 8)
        return combine(
            add, load_state(zin_ref.at[n]), correction(halo_of(i_y), yown_ref.at[n])
        )

    def announce(i, ref, state):
        store_state(ref, state)
        write_msg(msg_ref.at[i], state, deep=False)
        send_halo(i, ONE, 0)

    wait_round(R3, ONE, 8)
    announce(X2, x_ref.at[0], candidate(0, Y1, R3, own_ref.at[R3], False))
    announce(X3, x_ref.at[1], candidate(1, Y2, X2, x_ref.at[0], False))
    third = candidate(2, Y3, X3, x_ref.at[1], False)
    store_state(x_ref.at[2], third)

    gap = combine(lambda a, b: a - b, third, load_state(x_ref.at[1]))
    store_state(gap_ref, gap)
    write_msg(msg_ref.at[GAP], gap)
    store_state(x_ref.at[3], third)
    early = jnp.logical_and(t >= 1, t <= n_tm - 4)
    late = jnp.logical_or(t == 0, t >= n_tm - 3)

    @pl.when(early)
    def _():
        send_halo(GAP, TWO, 4, gap_sem.at[0])
        send_state(GAP, gap_ref, 4, gap_sem.at[0])

    @pl.when(late)
    def _():
        wait_round(GAP, TWO, 8)
        state = load_state(own_ref.at[GAP])
        p, d = unpack(halo_of(GAP), state[0], divergence(state), state[3][1], 2)
        values, _ = steps(p, d, 8 * DT, 2)
        total = {j: values[0][j] + values[1][j] for j in range(0, 3)}
        behind = [[values[2][0], values[2][1]], [None] * 2, [None] * 2, [None] * 2]
        for z in range(2):
            for c, slope in enumerate(grad(total, z)):
                behind[c + 1][z] = state[c + 1][z] - (8 * DT) * slope
        store_state(x_ref.at[3], combine(add, load_state(x_ref.at[2]), behind))

    write_msg(msg_ref.at[X4], load_state(x_ref.at[3]), deep=False)
    send_halo(X4, ONE, 0)
    levels = candidate(3, Y4, X4, x_ref.at[3], True)

    final = combine(add, load_state(rel_ref), levels)
    store_state(fin_ref, final)
    write_msg(msg_ref.at[LAST], final)
    send_halo(LAST, THREE, 1)
    send_state(LAST, fin_ref, 1)
    share_products(4, fin_ref)
    store_state(states_ref.at[3], final)
    wait_round(LAST, THREE, 8)
    state = load_state(own_ref.at[LAST])
    p, d = unpack(halo_of(LAST), state[0], divergence(state), state[3][1], 3)
    values, _ = steps(p, d, DT, 3, forced=True)
    for n in range(3):
        for z in range(2):
            state[0][z] = values[n + 1][z]
            for c, slope in enumerate(grad(values[n], z)):
                state[c + 1][z] = state[c + 1][z] - DT * slope
        store_state(states_ref.at[n], state)
    coords_ref[...] = to_row(solved(4))[:, :rank]

    with jax.named_scope("wait_sends"):
        wait_planes(send_sem.at[0], sum(sent) // math.prod(plane))
        for i in range(5):
            part = ar_ref.at[i, pl.ds(0, n_space - 1)]
            pltpu.make_async_copy(part, part, ar_send_sem.at[i]).wait()

        @pl.when(early)
        def _():
            wait_planes(gap_sem.at[0], planes_of(TWO) + 8)


def finish(states_ref, coords_ref, states_out, coords_out, sem):
    copies = [
        pltpu.make_async_copy(states_ref, states_out, sem.at[0]),
        pltpu.make_async_copy(coords_ref, coords_out, sem.at[1]),
    ]
    for copy in copies:
        copy.start()
    for copy in copies:
        copy.wait()


def body(n_tm, n_space, speed, forcing, guess, basis):
    rank = basis.shape[1]
    plane = speed.shape[1:]
    vmem = functools.partial(pltpu.VMEM, dtype=F32)
    dma = pltpu.SemaphoreType.DMA
    state = (4, 2, *plane)
    msg = (5, *plane)
    scratch = [
        vmem((rank, *state)),
        vmem((4, 2, plane[0], rank, plane[1])),
        vmem((rank, *msg)),
        vmem(state),
        vmem((2, *plane)),
        vmem((4, 2, *plane)),
        vmem((4, 2, *plane)),
        vmem((4, 3, 2, *plane)),
        vmem((8, *plane)),
        vmem((ROUNDS, *msg)),
        vmem((ROUNDS, 4, *msg)),
        vmem((ROUNDS, *state)),
        vmem((3, *msg)),
        vmem((4, *state)),
        vmem((3, *state)),
        vmem(state),
        vmem(state),
        vmem((4, *state)),
        vmem(state),
        vmem(state),
        vmem((5, n_space, 1, 128)),
        vmem((n_space, rank // 2, 128)),
        vmem((rank, 128)),
        vmem((rank, 128)),
        vmem((rank, 128)),
        dma((5,)),
        dma((1,)),
        dma((1,)),
        dma((ROUNDS,)),
        dma((5,)),
        dma((5,)),
        dma((1,)),
    ]
    done = pl.pallas_call(
        functools.partial(kernel, n_tm, n_space, rank),
        out_shape=(
            pltpu.VMEM((4, *state), F32),
            pltpu.VMEM((1, rank), F32),
        ),
        in_specs=[pl.BlockSpec(memory_space=pl.ANY)] * 4,
        out_specs=(
            pl.BlockSpec(memory_space=pltpu.VMEM),
            pl.BlockSpec(memory_space=pltpu.VMEM),
        ),
        scratch_shapes=scratch,
        compiler_params=pltpu.CompilerParams(collective_id=0, has_side_effects=True),
    )(speed, forcing, guess, basis)
    return pl.pallas_call(
        finish,
        out_shape=(
            jax.ShapeDtypeStruct((4, *state), F32),
            jax.ShapeDtypeStruct((1, rank), F32),
        ),
        in_specs=[pl.BlockSpec(memory_space=pltpu.VMEM)] * 2,
        out_specs=[pl.BlockSpec(memory_space=pl.ANY)] * 2,
        scratch_shapes=[dma((2,))],
    )(*(pltpu.with_memory_space_constraint(v, pltpu.VMEM) for v in done))


def solution(mesh):
    placed = (
        P("space", None, None),
        P("tm", "space", None, None),
        P("tm", None, "space", None, None),
        P("tm", None, None, "space", None, None),
    )
    return jax.shard_map(
        functools.partial(body, mesh.shape["tm"], mesh.shape["space"]),
        mesh=mesh,
        in_specs=placed,
        out_specs=(P("tm", None, "space", None, None), P("tm", None)),
        check_vma=False,
    )
```

```python
import functools
import math

import jax
import jax.numpy as jnp
from jax import lax
from jax.experimental import pallas as pl
from jax.experimental.pallas import tpu as pltpu
from jax.sharding import PartitionSpec as P

DT = 0.045
MESH = pl.DeviceIdType.MESH
F32 = jnp.float32

R1, R2, R3, Y1, Y2, Y3, Y4, X2, X3, X4, GAP, LAST = range(12)
ROUNDS = 12

DEEP = ((0, 5), (0, 5), (1, 5), (0, 3))
THREE = ((0, 5), (0, 5), (2, 4), (1, 2))
TWO = ((1, 5), (0, 3))
ONE = ((2, 4), (1, 2))
OFFSETS = (1, -1, 2, -2)


def kernel(
    n_tm,
    n_space,
    rank,
    speed_hbm,
    forcing_hbm,
    guess_hbm,
    basis_hbm,
    states_ref,
    coords_ref,
    b_ref,
    bt_ref,
    bm_ref,
    guess_ref,
    speed_ref,
    force_ref,
    speed_halo,
    force_halo,
    c2_ref,
    msg_ref,
    halo_ref,
    own_ref,
    yown_ref,
    zout_ref,
    zin_ref,
    rel_ref,
    res_ref,
    x_ref,
    gap_ref,
    fin_ref,
    dual_ref,
    ar_ref,
    gram_ref,
    inv_ref,
    part_ref,
    w_ref,
    local_sem,
    send_sem,
    gap_sem,
    recv_sem,
    ar_send_sem,
    ar_sem,
    gram_sem,
):
    plane = guess_ref.shape[2:]
    t = lax.axis_index("tm")
    s = lax.axis_index("space")

    def at_t(d):
        return lax.rem(t + (d + n_tm), n_tm)

    def at_s(d):
        return lax.rem(s + (d + n_space), n_space)

    loads = [
        pltpu.make_async_copy(guess_hbm.at[0], guess_ref, local_sem.at[0]),
        pltpu.make_async_copy(speed_hbm, speed_ref, local_sem.at[1]),
        pltpu.make_async_copy(forcing_hbm, force_ref, local_sem.at[2]),
        pltpu.make_async_copy(basis_hbm.at[0], b_ref, local_sem.at[3]),
    ]
    for load in loads:
        load.start()

    def start_rows(m, carry):
        c = m // 2
        z = lax.rem(m, 2)
        for x in range(plane[0]):
            pltpu.make_async_copy(
                basis_hbm.at[0, :, c, z, x, :], bt_ref.at[c, z, x], local_sem.at[4]
            ).start()
        return carry

    barrier = pltpu.get_barrier_semaphore()
    peers = [(dt, ds) for dt in (1, -1) for ds in (-2, -1, 0, 1, 2)]
    peers += [(4, ds) for ds in (-1, 0, 1)]
    peers += [(0, ds) for ds in range(1, n_space)]
    with jax.named_scope("signals"):
        for dt, ds in peers:
            pl.semaphore_signal(
                barrier, inc=1, device_id=(at_t(dt), at_s(ds)), device_id_type=MESH
            )
    with jax.named_scope("rows"):
        lax.fori_loop(0, 8, start_rows, 0)

    sent = []

    def words(ref):
        return math.prod(ref.shape)

    def send(src, dst, rsem, dt, ds, ssem=None):
        pltpu.make_async_remote_copy(
            src_ref=src,
            dst_ref=dst,
            send_sem=send_sem.at[0] if ssem is None else ssem,
            recv_sem=rsem,
            device_id=(at_t(dt), at_s(ds)),
            device_id_type=MESH,
        ).start()
        if ssem is None:
            sent.append(words(src))

    def wait_planes(sem, planes):
        part = bm_ref.reshape(rank * 5, *plane).at[pl.ds(0, planes)]
        pltpu.make_async_copy(part, part, sem).wait()

    ix = lax.broadcasted_iota(jnp.int32, plane, 0)
    iy = lax.broadcasted_iota(jnp.int32, plane, 1)
    nx, ny = plane
    zero = jnp.zeros(plane, F32)
    x_low, x_high = ix == 0, ix == nx - 1
    y_low, y_high = iy == 0, iy == ny - 1
    weight = 5.0 - x_low.astype(F32) - y_low.astype(F32)

    def x_ahead(v):
        return jnp.where(x_high, zero, pltpu.roll(v, nx - 1, 0))

    def x_behind(v):
        return jnp.where(x_low, zero, pltpu.roll(v, 1, 0))

    def y_ahead(v):
        return jnp.where(y_high, zero, pltpu.roll(v, ny - 1, 1))

    def y_behind(v):
        return jnp.where(y_low, zero, pltpu.roll(v, 1, 1))

    def flag(cond):
        return jnp.where(cond, 1.0, 0.0).astype(F32)

    e_dn1, e_dn2 = flag(s >= 1), flag(s >= 2)
    e_up1, e_up2 = flag(s <= n_space - 2), flag(s <= n_space - 3)
    floor = {0: e_dn1, -2: e_dn2}

    def lap(p, j):
        below = p[j - 1] - p[j]
        if j in floor:
            below = below * floor[j]
        return (
            (x_ahead(p[j]) + x_behind(p[j]))
            + (y_ahead(p[j]) + y_behind(p[j]))
            + (p[j + 1] - weight * p[j])
            + below
        )

    def c2(j):
        return c2_ref[j + 3]

    def force(n, j):
        if j in (0, 1):
            return force_ref[n, j]
        if j in (-1, -2):
            return force_halo[0, n, j + 2] * e_dn1
        if j in (2, 3):
            return force_halo[1, n, j - 2] * e_up1
        if j == -3:
            return force_halo[2, 0, 1] * e_dn2
        return force_halo[3, 0, 0] * e_up2

    def steps(p, d, h, count, forced=False):
        values, first = [p], None
        for n in range(count):
            depth = count - 1 - n
            planes = range(-depth, 2 + depth)
            laps = {j: lap(p, j) for j in planes}
            if first is None:
                first = laps
            d = {j: d[j] - h * laps[j] for j in planes}
            p = {j: p[j] - (h * c2(j)) * d[j] for j in planes}
            if forced:
                p = {j: p[j] + force(n, j) for j in planes}
            values.append(p)
        return values, first

    def grad(p, j):
        return (x_ahead(p[j]) - p[j], y_ahead(p[j]) - p[j], p[j + 1] - p[j])

    def divergence(state):
        both = []
        for z in range(2):
            both.append(
                (state[1][z] - x_behind(state[1][z]))
                + (state[2][z] - y_behind(state[2][z]))
            )
        return both[0] + state[3][0], both[1] + (state[3][1] - state[3][0])

    def load_state(ref):
        return [[ref[c, z] for z in range(2)] for c in range(4)]

    def store_state(ref, state):
        for c in range(4):
            for z in range(2):
                ref[c, z] = state[c][z]

    def combine(fn, *states):
        return [[fn(*[u[c][z] for u in states]) for z in range(2)] for c in range(4)]

    def write_msg(ref, state, deep=True):
        if deep:
            low, high = divergence(state)
            ref[0] = low
            ref[4] = high
        ref[1] = state[0][0]
        ref[2] = state[0][1]
        ref[3] = state[3][1]

    def unpack(halo, own_p, own_d, own_vz, depth):
        p = {0: own_p[0], 1: own_p[1]}
        vz_below = halo[0, 3] * e_dn1
        p[-1] = halo[0, 2] * e_dn1
        p[2] = halo[1, 1] * e_up1
        d = {0: own_d[0] - vz_below, 1: own_d[1]}
        if depth >= 2:
            p[-2] = halo[0, 1] * e_dn1
            p[3] = halo[1, 2] * e_up1
            d[-1] = halo[0, 4]
            d[2] = halo[1, 0] - own_vz
        if depth >= 3:
            p[-3] = halo[2, 2] * e_dn2
            p[4] = halo[3, 1] * e_up2
            d[-2] = halo[0, 0] - halo[2, 3] * e_dn2
            d[3] = halo[1, 4]
        if depth >= 4:
            p[-4] = halo[2, 1] * e_dn2
            p[5] = halo[3, 2] * e_up2
            d[-3] = halo[2, 4]
            d[4] = halo[3, 0] - halo[1, 3]
        return p, d

    def send_halo(i, slices, dt, ssem=None):
        for k in reversed(range(len(slices))):
            low, high = slices[k]
            part = pl.ds(low, high - low)
            send(
                msg_ref.at[i, part],
                halo_ref.at[i, k, part],
                recv_sem.at[i],
                dt,
                OFFSETS[k],
                ssem,
            )

    def planes_of(slices):
        return sum(high - low for low, high in slices)

    def send_own(i, src, dst, dt, ssem=None):
        send(src, dst, recv_sem.at[i], dt, 0, ssem)

    def send_state(i, ref, dt, ssem=None):
        send_own(i, ref, own_ref.at[i], dt, ssem)

    def wait_round(i, slices, more):
        with jax.named_scope(f"wait_round{i}"):
            wait_planes(recv_sem.at[i], planes_of(slices) + more)

    def halo_of(i):
        return halo_ref.at[i]

    rows = lax.broadcasted_iota(jnp.int32, (rank, 128), 0)
    lanes = lax.broadcasted_iota(jnp.int32, (rank, 128), 1)
    diagonal = rows == lanes

    far_first = sorted(range(1, n_space), key=lambda j: abs(abs(j - n_space // 2) - 2))

    def to_row(column):
        spread = jnp.where(diagonal, jnp.broadcast_to(column, (rank, 128)), 0.0)
        return jnp.sum(spread, axis=0, keepdims=True)

    def products(name, columns, field, planes, more=False):
        with jax.named_scope(name):
            out = []
            for r in range(rank):
                total = None
                for at in planes:
                    for half in range(nx // 8):
                        part = (*at, slice(half * 8, half * 8 + 8), slice(None))
                        term = columns[(r, *part)] * field[part]
                        total = term if total is None else total + term
                out.append(jnp.sum(total, axis=0, keepdims=True))
                if r % 8 == 7:
                    block = jnp.concatenate(out, axis=0)
                    if more:
                        block = block + part_ref[r - 7 : r + 1, :]
                    part_ref[r - 7 : r + 1, :] = block
                    out = []

    def full_products(name, field, more=False):
        products(name, b_ref, field, [(c, z) for c in range(4) for z in range(2)], more)

    def dual_products(name):
        products(name, bm_ref, dual_ref, [(m,) for m in range(5)], True)

    def share_products(i):
        with jax.named_scope(f"share{i}"):
            ar_ref[i, s] = to_row(jnp.sum(part_ref[...], axis=1, keepdims=True))
            for j in far_first:
                send(ar_ref.at[i, s], ar_ref.at[i, s], ar_sem.at[i], 0, j, ar_send_sem.at[i])

    def solved(i):
        with jax.named_scope(f"wait_ar{i}"):
            part = ar_ref.at[i, pl.ds(0, n_space - 1)]
            pltpu.make_async_copy(part, part, ar_sem.at[i]).wait()
        total = ar_ref[i, 0]
        for j in range(1, n_space):
            total = total + ar_ref[i, j]
        return jnp.sum(inv_ref[...] * total, axis=1, keepdims=True)

    def combine_columns(i, weights):
        w_ref[...] = jnp.broadcast_to(weights, (rank, 128))

        def group(g, acc):
            for k in range(16):
                r = g * 16 + k
                w = jnp.broadcast_to(w_ref[pl.ds(r, 1), :], plane)
                acc = tuple(acc[m] + w * bm_ref[r, m] for m in range(5))
            return acc

        with jax.named_scope(f"columns{i}"):
            acc = lax.fori_loop(0, rank // 16, group, (zero,) * 5)
            for m in range(5):
                msg_ref[i, m] = acc[m]

    def eliminate(low, high):
        def step(i, carry):
            k = 2 * i
            at0, at1 = lanes == 128 - rank + k, lanes == 128 - rank + k + 1

            def pick(mask, v):
                return jnp.sum(jnp.where(mask, v, 0.0), axis=1, keepdims=True)

            m = inv_ref[...]
            row0, row1 = inv_ref[pl.ds(k, 1), :], inv_ref[pl.ds(k + 1, 1), :]
            col0, col1 = pick(at0, m), pick(at1, m)
            a, b = pick(at0[0:1], row0), pick(at1[0:1], row0)
            c, d = pick(at0[0:1], row1), pick(at1[0:1], row1)
            ratio = b / a
            row0 = row0 / a
            row1 = (row1 - c * row0) / (d - c * ratio)
            row0 = row0 - ratio * row1
            m = (m - col0 * row0) - col1 * row1
            m = jnp.where(rows == k, row0, m)
            inv_ref[...] = jnp.where(rows == k + 1, row1, m)
            return carry

        with jax.named_scope(f"eliminate{low}"):
            lax.fori_loop(low // 2, high // 2, step, 0)

    def wait_rows():
        with jax.named_scope("wait_bt"):
            pltpu.make_async_copy(bt_ref, bt_ref, local_sem.at[4]).wait()

    def gram_part(i, acc):
        c = i // 4
        z = lax.rem(i // 2, 2)
        x = lax.rem(i, 2) * 8
        flat = jnp.concatenate([bt_ref[c, z, x + k] for k in range(8)], axis=1)
        high = flat.astype(jnp.bfloat16)
        rest = flat - high.astype(F32)
        middle = rest.astype(jnp.bfloat16)
        low = (rest - middle.astype(F32)).astype(jnp.bfloat16)
        stacked = jnp.concatenate([high, middle, low], axis=0)
        return acc + lax.dot_general(
            stacked,
            stacked,
            (((1,), (1,)), ((), ())),
            preferred_element_type=F32,
        )

    each = rank // n_space

    def send_gram():
        with jax.named_scope("gram"):
            acc = lax.fori_loop(0, 16, gram_part, jnp.zeros((3 * rank, 3 * rank), F32))
        acc = acc[2 * rank :] + acc[rank : 2 * rank] + acc[:rank]
        gram = acc[:, 2 * rank :] + acc[:, rank : 2 * rank] + acc[:, :rank]
        gram = jnp.concatenate([jnp.zeros((rank, 128 - rank), F32), gram], axis=1)
        for o in range(n_space):
            gram_ref[0, o] = gram[o * each : o * each + each]
        gram_ref[1, s] = gram_ref[0, s]
        for j in far_first:
            send(
                gram_ref.at[0, at_s(j)], gram_ref.at[1, s], gram_sem.at[0], 0, j, gram_sem.at[2]
            )

    def wait_gram(k):
        with jax.named_scope(f"wait_gram{k}"):
            part = gram_ref.at[1, pl.ds(0, n_space - 1)]
            pltpu.make_async_copy(part, part, gram_sem.at[k]).wait()

    def share_gram():
        wait_gram(0)
        rows_sum = gram_ref[1, 0]
        for o in range(1, n_space):
            rows_sum = rows_sum + gram_ref[1, o]
        gram_ref[2, s] = rows_sum
        for j in far_first:
            send(
                gram_ref.at[2, s], gram_ref.at[2, s], gram_sem.at[1], 0, j, gram_sem.at[3]
            )

    with jax.named_scope("barrier"):
        pl.semaphore_wait(barrier, len(peers))

    with jax.named_scope("wait_guess"):
        loads[0].wait()
    write_msg(msg_ref.at[R1], load_state(guess_ref))
    send_halo(R1, DEEP, 1)
    send_state(R1, guess_ref, 1)
    with jax.named_scope("wait_load12"):
        loads[1].wait()
        loads[2].wait()
    edge = (None, None, pl.ds(1, 1), pl.ds(0, 1))
    for k in (3, 2, 1, 0):
        if edge[k] is None:
            pair = [
                (speed_ref, speed_halo.at[k]),
                (force_ref.at[pl.ds(0, 2)], force_halo.at[k, pl.ds(0, 2)]),
                (force_ref.at[2, pl.ds(1 - k, 1)], force_halo.at[k, 2, pl.ds(1 - k, 1)]),
            ]
        else:
            pair = [
                (speed_ref.at[edge[k]], speed_halo.at[k, edge[k]]),
                (
                    force_ref.at[pl.ds(0, 1), edge[k]],
                    force_halo.at[k, pl.ds(0, 1), edge[k]],
                ),
            ]
        for src, dst in pair:
            send(src, dst, recv_sem.at[R1], 0, OFFSETS[k])

    wait_rows()
    send_gram()

    wait_round(R1, DEEP, 8 + 6 + 12)
    for j, value, on in (
        (0, speed_ref[0], None),
        (1, speed_ref[1], None),
        (-1, speed_halo[0, 1], e_dn1),
        (-2, speed_halo[0, 0], e_dn1),
        (2, speed_halo[1, 0], e_up1),
        (3, speed_halo[1, 1], e_up1),
        (-3, speed_halo[2, 1], e_dn2),
        (4, speed_halo[3, 0], e_up2),
    ):
        squared = value * value
        c2_ref[j + 3] = squared if on is None else squared * on

    def four_forced(i):
        state = load_state(own_ref.at[i])
        low, high = divergence(state)
        p, d = unpack(halo_of(i), state[0], (low, high), state[3][1], 4)
        values, _ = steps(p, d, DT, 4, forced=True)
        total = {
            j: (values[0][j] + values[1][j]) + (values[2][j] + values[3][j])
            for j in range(0, 3)
        }
        out = [[values[4][0], values[4][1]], [None] * 2, [None] * 2, [None] * 2]
        for z in range(2):
            for c, slope in enumerate(grad(total, z)):
                out[c + 1][z] = state[c + 1][z] - DT * slope
        return out

    relaxed = four_forced(R1)
    store_state(rel_ref, relaxed)
    write_msg(msg_ref.at[R2], relaxed)
    send_halo(R2, DEEP, 1)
    send_state(R2, rel_ref, 1)

    with jax.named_scope("wait_basis"):
        loads[3].wait()

    def column_msg(g, carry):
        for k in range(8):
            write_msg(bm_ref.at[g * 8 + k], load_state(b_ref.at[g * 8 + k]))
        return carry

    with jax.named_scope("column_msg"):
        lax.fori_loop(0, rank // 8, column_msg, 0)
    share_gram()
    wait_round(R2, DEEP, 8)
    residue = combine(lambda a, b: a - b, four_forced(R2), load_state(rel_ref))
    store_state(res_ref, residue)
    write_msg(msg_ref.at[R3], residue, deep=False)
    send(res_ref, own_ref.at[R3], recv_sem.at[ROUNDS], 1, 0)
    send_halo(R3, ONE, 1)


    def coarse(state, halo):
        p, d = unpack(halo, state[0], divergence(state), None, 1)
        values, _ = steps(p, d, 4 * DT, 1)
        out = [[values[1][0], values[1][1]], [None] * 2, [None] * 2, [None] * 2]
        for z in range(2):
            for c, slope in enumerate(grad(p, z)):
                out[c + 1][z] = state[c + 1][z] - (4 * DT) * slope
        return out

    def correction(halo, own):
        p, d = unpack(halo, (own[1], own[2]), (own[0], own[4]), own[3], 4)
        values, first = steps(p, d, DT, 4)
        moved = []
        for z in range(2):
            slow = p[z] - (4 * DT * c2(z)) * (d[z] - (4 * DT) * first[z])
            moved.append(values[4][z] - slow)
        total = {
            j: (values[1][j] - p[j]) + (values[2][j] - p[j]) + (values[3][j] - p[j])
            for j in range(0, 3)
        }
        dual = (DT * total[0], moved[0], moved[1], -DT * total[2], DT * total[1])
        for m in range(5):
            dual_ref[m] = dual[m]
        return moved, total

    def corrected(state, moved, total):
        out = [[state[0][z] + moved[z] for z in range(2)], [None] * 2, [None] * 2, [None] * 2]
        for z in range(2):
            for c, slope in enumerate(grad(total, z)):
                out[c + 1][z] = state[c + 1][z] - DT * slope
        return out

    def add(a, b):
        return a + b

    def candidate(n, i_y, i_x, x_state_ref):
        last = i_y == Y4
        if n == 0:
            invert_gram()
        wait_round(i_x, ONE, 0)
        z = combine(add, coarse(load_state(x_state_ref), halo_of(i_x)), load_state(res_ref))
        if last:
            store_state(fin_ref, combine(add, z, load_state(rel_ref)))
        else:
            store_state(zout_ref.at[n], z)
            send(zout_ref.at[n], zin_ref.at[n], recv_sem.at[ROUNDS + 1 + n], 1, 0)
        combine_columns(i_y, solved(n))
        send_halo(i_y, DEEP, 0 if last else 1)
        if last:
            full_products("products_last", fin_ref)
            wait_round(i_y, DEEP, 0)
            return correction(halo_of(i_y), msg_ref.at[i_y])
        send_own(i_y, msg_ref.at[i_y], yown_ref.at[n], 1)
        with jax.named_scope(f"wait_z{n}"):
            wait_planes(recv_sem.at[ROUNDS + 1 + n], 8)
        full_products(f"products_z{n}", zin_ref.at[n])
        wait_round(i_y, DEEP, 5)
        return correction(halo_of(i_y), yown_ref.at[n])

    def invert_gram():
        wait_gram(1)
        for o in range(n_space):
            inv_ref[o * each : o * each + each, :] = gram_ref[2, o]
        inv_ref[...] = inv_ref[...] + diagonal.astype(F32)
        eliminate(0, rank)

    def announce(i, state_ref, moved, total):
        msg_ref[i, 1] = state_ref[0, 0] + moved[0]
        msg_ref[i, 2] = state_ref[0, 1] + moved[1]
        msg_ref[i, 3] = state_ref[3, 1] - DT * (total[2] - total[1])
        send_halo(i, ONE, 0)

    with jax.named_scope("wait_res"):
        wait_planes(recv_sem.at[ROUNDS], 8)
    full_products("products0", own_ref.at[R3])
    share_products(0)
    for n, (i_y, i_x, ref) in enumerate(
        ((Y1, R3, own_ref.at[R3]), (Y2, X2, x_ref.at[0]))
    ):
        moved, total = candidate(n, i_y, i_x, ref)
        announce(X2 + n, zin_ref.at[n], moved, total)
        dual_products(f"products{n + 1}")
        share_products(n + 1)
        store_state(x_ref.at[n], corrected(load_state(zin_ref.at[n]), moved, total))
    moved, total = candidate(2, Y3, X3, x_ref.at[1])
    third = corrected(load_state(zin_ref.at[2]), moved, total)

    gap = combine(lambda a, b: a - b, third, load_state(x_ref.at[1]))
    store_state(gap_ref, gap)
    write_msg(msg_ref.at[GAP], gap)
    early = jnp.logical_and(t >= 1, t <= n_tm - 4)
    late = jnp.logical_or(t == 0, t >= n_tm - 3)

    @pl.when(early)
    def _():
        send_halo(GAP, TWO, 4, gap_sem.at[0])
        send_state(GAP, gap_ref, 4, gap_sem.at[0])

    store_state(x_ref.at[2], third)
    dual_products("products3")

    @pl.when(late)
    def _():
        wait_round(GAP, TWO, 8)
        state = load_state(own_ref.at[GAP])
        p, d = unpack(halo_of(GAP), state[0], divergence(state), state[3][1], 2)
        values, _ = steps(p, d, 8 * DT, 2)
        total = {j: values[0][j] + values[1][j] for j in range(0, 3)}
        behind = [[values[2][0], values[2][1]], [None] * 2, [None] * 2, [None] * 2]
        for z in range(2):
            for c, slope in enumerate(grad(total, z)):
                behind[c + 1][z] = state[c + 1][z] - (8 * DT) * slope
        store_state(x_ref.at[3], behind)
        store_state(x_ref.at[2], combine(add, load_state(x_ref.at[2]), behind))

    write_msg(msg_ref.at[X4], load_state(x_ref.at[2]), deep=False)
    send_halo(X4, ONE, 0)

    @pl.when(late)
    def _():
        full_products("products_gap", x_ref.at[3], True)

    share_products(3)
    moved, total = candidate(3, Y4, X4, x_ref.at[2])

    final = corrected(load_state(fin_ref), moved, total)
    store_state(fin_ref, final)
    write_msg(msg_ref.at[LAST], final)
    send_halo(LAST, THREE, 1)
    send_state(LAST, fin_ref, 1)
    dual_products("products4")
    share_products(4)
    store_state(states_ref.at[3], final)
    wait_round(LAST, THREE, 8)
    state = load_state(own_ref.at[LAST])
    p, d = unpack(halo_of(LAST), state[0], divergence(state), state[3][1], 3)
    values, _ = steps(p, d, DT, 3, forced=True)
    for n in range(3):
        for z in range(2):
            state[0][z] = values[n + 1][z]
            for c, slope in enumerate(grad(values[n], z)):
                state[c + 1][z] = state[c + 1][z] - DT * slope
        store_state(states_ref.at[n], state)
    coords_ref[...] = to_row(solved(4))[:, :rank]

    with jax.named_scope("wait_sends"):
        planes, odd = divmod(sum(sent), math.prod(plane))
        assert odd == 0
        wait_planes(send_sem.at[0], planes)
        for k in (2, 3):
            wait_gram(k)
        for i in range(5):
            part = ar_ref.at[i, pl.ds(0, n_space - 1)]
            pltpu.make_async_copy(part, part, ar_send_sem.at[i]).wait()

        @pl.when(early)
        def _():
            wait_planes(gap_sem.at[0], planes_of(TWO) + 8)


def finish(states_ref, coords_ref, states_out, coords_out, sem):
    copies = [
        pltpu.make_async_copy(states_ref, states_out, sem.at[0]),
        pltpu.make_async_copy(coords_ref, coords_out, sem.at[1]),
    ]
    for copy in copies:
        copy.start()
    for copy in copies:
        copy.wait()


def body(n_tm, n_space, speed, forcing, guess, basis):
    rank = basis.shape[1]
    plane = speed.shape[1:]
    vmem = functools.partial(pltpu.VMEM, dtype=F32)
    dma = pltpu.SemaphoreType.DMA
    state = (4, 2, *plane)
    msg = (5, *plane)
    scratch = [
        vmem((rank, *state)),
        vmem((4, 2, plane[0], rank, plane[1])),
        vmem((rank, *msg)),
        vmem(state),
        vmem((2, *plane)),
        vmem((4, 2, *plane)),
        vmem((4, 2, *plane)),
        vmem((4, 3, 2, *plane)),
        vmem((8, *plane)),
        vmem((ROUNDS, *msg)),
        vmem((ROUNDS, 4, *msg)),
        vmem((ROUNDS, *state)),
        vmem((3, *msg)),
        vmem((4, *state)),
        vmem((3, *state)),
        vmem(state),
        vmem(state),
        vmem((4, *state)),
        vmem(state),
        vmem(state),
        vmem(msg),
        vmem((5, n_space, 1, 128)),
        vmem((3, n_space, rank // n_space, 128)),
        vmem((rank, 128)),
        vmem((rank, 128)),
        vmem((rank, 128)),
        dma((5,)),
        dma((1,)),
        dma((1,)),
        dma((ROUNDS + 4,)),
        dma((5,)),
        dma((5,)),
        dma((4,)),
    ]
    done = pl.pallas_call(
        functools.partial(kernel, n_tm, n_space, rank),
        out_shape=(
            pltpu.VMEM((4, *state), F32),
            pltpu.VMEM((1, rank), F32),
        ),
        in_specs=[pl.BlockSpec(memory_space=pl.ANY)] * 4,
        out_specs=(
            pl.BlockSpec(memory_space=pltpu.VMEM),
            pl.BlockSpec(memory_space=pltpu.VMEM),
        ),
        scratch_shapes=scratch,
        compiler_params=pltpu.CompilerParams(collective_id=0, has_side_effects=True),
    )(speed, forcing, guess, basis)
    return pl.pallas_call(
        finish,
        out_shape=(
            jax.ShapeDtypeStruct((4, *state), F32),
            jax.ShapeDtypeStruct((1, rank), F32),
        ),
        in_specs=[pl.BlockSpec(memory_space=pltpu.VMEM)] * 2,
        out_specs=[pl.BlockSpec(memory_space=pl.ANY)] * 2,
        scratch_shapes=[dma((2,))],
    )(*(pltpu.with_memory_space_constraint(v, pltpu.VMEM) for v in done))


def solution(mesh):
    placed = (
        P("space", None, None),
        P("tm", "space", None, None),
        P("tm", None, "space", None, None),
        P("tm", None, None, "space", None, None),
    )
    return jax.shard_map(
        functools.partial(body, mesh.shape["tm"], mesh.shape["space"]),
        mesh=mesh,
        in_specs=placed,
        out_specs=(P("tm", None, "space", None, None), P("tm", None)),
        check_vma=False,
    )
```

```python
import functools
import math

import jax
import jax.numpy as jnp
from jax import lax
from jax.experimental import pallas as pl
from jax.experimental.pallas import tpu as pltpu
from jax.sharding import PartitionSpec as P

DT = 0.045
MESH = pl.DeviceIdType.MESH
F32 = jnp.float32

R1, R2, R3, Y1, Y2, Y3, Y4, X2, X3, X4, GAP, LAST = range(12)
ROUNDS = 12

DEEP = ((0, 5), (0, 5), (1, 5), (0, 3))
THREE = ((0, 5), (0, 5), (2, 4), (1, 2))
TWO = ((1, 5), (0, 3))
ONE = ((2, 4), (1, 2))
OFFSETS = (1, -1, 2, -2)


def kernel(
    n_tm,
    n_space,
    rank,
    speed_hbm,
    forcing_hbm,
    guess_hbm,
    basis_hbm,
    states_ref,
    coords_ref,
    b_ref,
    bt_ref,
    bm_ref,
    guess_ref,
    speed_ref,
    force_ref,
    speed_halo,
    force_halo,
    c2_ref,
    msg_ref,
    halo_ref,
    own_ref,
    yown_ref,
    zout_ref,
    zin_ref,
    rel_ref,
    res_ref,
    x_ref,
    gap_ref,
    fin_ref,
    dual_ref,
    ar_ref,
    gram_ref,
    inv_ref,
    part_ref,
    w_ref,
    local_sem,
    send_sem,
    gap_sem,
    recv_sem,
    ar_send_sem,
    ar_sem,
    gram_sem,
):
    plane = guess_ref.shape[2:]
    t = lax.axis_index("tm")
    s = lax.axis_index("space")

    def at_t(d):
        return lax.rem(t + (d + n_tm), n_tm)

    def at_s(d):
        return lax.rem(s + (d + n_space), n_space)

    inner = jnp.logical_and(s >= 2, s <= n_space - 3)
    edge = jnp.logical_not(inner)
    has = {0: None, 1: s <= n_space - 2, -1: s >= 1, 2: s <= n_space - 3, -2: s >= 2}
    edges = ((0, (-1, -2)), (1, (-2,)), (n_space - 2, (2,)), (n_space - 1, (1, 2)))

    def where_it_is(act):
        @pl.when(inner)
        def _():
            act(())

        @pl.when(edge)
        def _():
            for place, out in edges:

                @pl.when(s == place)
                def _(out=out):
                    act(out)

    loads = [
        pltpu.make_async_copy(guess_hbm.at[0], guess_ref, local_sem.at[0]),
        pltpu.make_async_copy(speed_hbm, speed_ref, local_sem.at[1]),
        pltpu.make_async_copy(forcing_hbm, force_ref, local_sem.at[2]),
        pltpu.make_async_copy(basis_hbm.at[0], b_ref, local_sem.at[3]),
    ]
    for load in loads:
        load.start()

    far_first = sorted(range(1, n_space), key=lambda j: abs(abs(j - n_space // 2) - 2))

    def start_rows(m, carry):
        c = m // 2
        z = lax.rem(m, 2)
        for x in range(plane[0]):
            pltpu.make_async_copy(
                basis_hbm.at[0, :, c, z, x, :], bt_ref.at[c, z, x], local_sem.at[4]
            ).start()
        return carry

    @pl.when(edge)
    def _():
        def clear(i, carry):
            for k in range(4):
                for m in range(5):
                    halo_ref[i, k, m] = jnp.zeros(plane, F32)
            return carry

        lax.fori_loop(0, ROUNDS, clear, 0)
        for k in range(4):
            for z in range(2):
                speed_halo[k, z] = jnp.zeros(plane, F32)
                for n in range(3):
                    force_halo[k, n, z] = jnp.zeros(plane, F32)

    barrier = pltpu.get_barrier_semaphore()
    count = 0
    with jax.named_scope("signals"):

        def greet(dt, ds):
            pl.semaphore_signal(
                barrier, inc=1, device_id=(at_t(dt), at_s(ds)), device_id_type=MESH
            )

        for ds in (2, -2, 1, -1, 0):
            near = (1, -1, 4) if abs(ds) < 2 else (1, -1)
            if has[ds] is None:
                count = count + len(near)
                for dt in near:
                    greet(dt, ds)
            else:
                count = count + len(near) * has[ds].astype(jnp.int32)

                @pl.when(has[ds])
                def _(near=near, ds=ds):
                    for dt in near:
                        greet(dt, ds)

        for ds in far_first:
            count = count + 1
            greet(0, ds)
    with jax.named_scope("rows"):
        lax.fori_loop(0, 8, start_rows, 0)

    sent = {offset: 0 for offset in has}

    def words(ref):
        return math.prod(ref.shape)

    def send(src, dst, rsem, dt, ds, ssem=None, tally=True):
        pltpu.make_async_remote_copy(
            src_ref=src,
            dst_ref=dst,
            send_sem=send_sem.at[0] if ssem is None else ssem,
            recv_sem=rsem,
            device_id=(at_t(dt), at_s(ds)),
            device_id_type=MESH,
        ).start()
        if ssem is None and tally:
            sent[ds] += words(src)

    def wait_planes(sem, planes):
        part = bm_ref.reshape(rank * 5, *plane).at[pl.ds(0, planes)]
        pltpu.make_async_copy(part, part, sem).wait()

    ix = lax.broadcasted_iota(jnp.int32, plane, 0)
    iy = lax.broadcasted_iota(jnp.int32, plane, 1)
    nx, ny = plane
    zero = jnp.zeros(plane, F32)
    x_low, x_high = ix == 0, ix == nx - 1
    y_low, y_high = iy == 0, iy == ny - 1
    weight = 5.0 - x_low.astype(F32) - y_low.astype(F32)

    def x_ahead(v):
        return jnp.where(x_high, zero, pltpu.roll(v, nx - 1, 0))

    def x_behind(v):
        return jnp.where(x_low, zero, pltpu.roll(v, 1, 0))

    def y_ahead(v):
        return jnp.where(y_high, zero, pltpu.roll(v, ny - 1, 1))

    def y_behind(v):
        return jnp.where(y_low, zero, pltpu.roll(v, 1, 1))

    def flag(cond):
        return jnp.where(cond, 1.0, 0.0).astype(F32)

    e_dn1, e_dn2 = flag(s >= 1), flag(s >= 2)
    e_up1, e_up2 = flag(s <= n_space - 2), flag(s <= n_space - 3)
    floor = {0: e_dn1, -2: e_dn2}

    def lap(p, j):
        below = p[j - 1] - p[j]
        if j in floor:
            below = below * floor[j]
        return (
            (x_ahead(p[j]) + x_behind(p[j]))
            + (y_ahead(p[j]) + y_behind(p[j]))
            + (p[j + 1] - weight * p[j])
            + below
        )

    def c2(j):
        return c2_ref[j + 3]

    def force(n, j):
        if j in (0, 1):
            return force_ref[n, j]
        if j in (-1, -2):
            return force_halo[0, n, j + 2] * e_dn1
        if j in (2, 3):
            return force_halo[1, n, j - 2] * e_up1
        if j == -3:
            return force_halo[2, 0, 1] * e_dn2
        return force_halo[3, 0, 0] * e_up2

    def steps(p, d, h, count, forced=False):
        values, first = [p], None
        for n in range(count):
            depth = count - 1 - n
            planes = range(-depth, 2 + depth)
            laps = {j: lap(p, j) for j in planes}
            if first is None:
                first = laps
            d = {j: d[j] - h * laps[j] for j in planes}
            p = {j: p[j] - (h * c2(j)) * d[j] for j in planes}
            if forced:
                p = {j: p[j] + force(n, j) for j in planes}
            values.append(p)
        return values, first

    def grad(p, j):
        return (x_ahead(p[j]) - p[j], y_ahead(p[j]) - p[j], p[j + 1] - p[j])

    def divergence(state):
        both = []
        for z in range(2):
            both.append(
                (state[1][z] - x_behind(state[1][z]))
                + (state[2][z] - y_behind(state[2][z]))
            )
        return both[0] + state[3][0], both[1] + (state[3][1] - state[3][0])

    def load_state(ref):
        return [[ref[c, z] for z in range(2)] for c in range(4)]

    def store_state(ref, state):
        for c in range(4):
            for z in range(2):
                ref[c, z] = state[c][z]

    def combine(fn, *states):
        return [[fn(*[u[c][z] for u in states]) for z in range(2)] for c in range(4)]

    def write_msg(ref, state, deep=True):
        if deep:
            low, high = divergence(state)
            ref[0] = low
            ref[4] = high
        ref[1] = state[0][0]
        ref[2] = state[0][1]
        ref[3] = state[3][1]

    def unpack(halo, own_p, own_d, own_vz, depth):
        p = {0: own_p[0], 1: own_p[1]}
        vz_below = halo[0, 3] * e_dn1
        p[-1] = halo[0, 2] * e_dn1
        p[2] = halo[1, 1] * e_up1
        d = {0: own_d[0] - vz_below, 1: own_d[1]}
        if depth >= 2:
            p[-2] = halo[0, 1] * e_dn1
            p[3] = halo[1, 2] * e_up1
            d[-1] = halo[0, 4]
            d[2] = halo[1, 0] - own_vz
        if depth >= 3:
            p[-3] = halo[2, 2] * e_dn2
            p[4] = halo[3, 1] * e_up2
            d[-2] = halo[0, 0] - halo[2, 3] * e_dn2
            d[3] = halo[1, 4]
        if depth >= 4:
            p[-4] = halo[2, 1] * e_dn2
            p[5] = halo[3, 2] * e_up2
            d[-3] = halo[2, 4]
            d[4] = halo[3, 0] - halo[1, 3]
        return p, d

    def send_halo(i, slices, dt, ssem=None):
        def act(out):
            for k in reversed(range(len(slices))):
                if OFFSETS[k] not in out:
                    low, high = slices[k]
                    part = pl.ds(low, high - low)
                    send(
                        msg_ref.at[i, part],
                        halo_ref.at[i, k, part],
                        recv_sem.at[i],
                        dt,
                        OFFSETS[k],
                        ssem,
                        out == (),
                    )

        where_it_is(act)

    def planes_of(slices, out=()):
        return sum(
            high - low for k, (low, high) in enumerate(slices) if -OFFSETS[k] not in out
        )

    def send_own(i, src, dst, dt, ssem=None):
        send(src, dst, recv_sem.at[i], dt, 0, ssem)

    def send_state(i, ref, dt, ssem=None):
        send_own(i, ref, own_ref.at[i], dt, ssem)

    def wait_round(i, slices, more):
        with jax.named_scope(f"wait_round{i}"):
            where_it_is(
                lambda out: wait_planes(recv_sem.at[i], planes_of(slices, out) + more)
            )

    def halo_of(i):
        return halo_ref.at[i]

    rows = lax.broadcasted_iota(jnp.int32, (rank, 128), 0)
    lanes = lax.broadcasted_iota(jnp.int32, (rank, 128), 1)
    diagonal = rows == lanes

    def to_row(column):
        spread = jnp.where(diagonal, jnp.broadcast_to(column, (rank, 128)), 0.0)
        return jnp.sum(spread, axis=0, keepdims=True)

    def products(name, columns, field, planes, more=False):
        with jax.named_scope(name):
            out = []
            for r in range(rank):
                total = None
                for at in planes:
                    for half in range(nx // 8):
                        part = (*at, slice(half * 8, half * 8 + 8), slice(None))
                        term = columns[(r, *part)] * field[part]
                        total = term if total is None else total + term
                out.append(jnp.sum(total, axis=0, keepdims=True))
                if r % 8 == 7:
                    block = jnp.concatenate(out, axis=0)
                    if more:
                        block = block + part_ref[r - 7 : r + 1, :]
                    part_ref[r - 7 : r + 1, :] = block
                    out = []

    def full_products(name, field, more=False):
        products(name, b_ref, field, [(c, z) for c in range(4) for z in range(2)], more)

    def dual_products(name):
        products(name, bm_ref, dual_ref, [(m,) for m in range(5)], True)

    def share_products(i):
        with jax.named_scope(f"share{i}"):
            ar_ref[i, s] = to_row(jnp.sum(part_ref[...], axis=1, keepdims=True))
            for j in far_first:
                send(ar_ref.at[i, s], ar_ref.at[i, s], ar_sem.at[i], 0, j, ar_send_sem.at[i])

    def solved(i):
        with jax.named_scope(f"wait_ar{i}"):
            part = ar_ref.at[i, pl.ds(0, n_space - 1)]
            pltpu.make_async_copy(part, part, ar_sem.at[i]).wait()
        total = ar_ref[i, 0]
        for j in range(1, n_space):
            total = total + ar_ref[i, j]
        return jnp.sum(inv_ref[...] * total, axis=1, keepdims=True)

    def combine_columns(i, weights):
        w_ref[...] = jnp.broadcast_to(weights, (rank, 128))

        def group(g, acc):
            for k in range(16):
                r = g * 16 + k
                w = jnp.broadcast_to(w_ref[pl.ds(r, 1), :], plane)
                acc = tuple(acc[m] + w * bm_ref[r, m] for m in range(5))
            return acc

        with jax.named_scope(f"columns{i}"):
            acc = lax.fori_loop(0, rank // 16, group, (zero,) * 5)
            for m in range(5):
                msg_ref[i, m] = acc[m]

    def eliminate(low, high):
        def step(i, carry):
            k = 2 * i
            at0, at1 = lanes == 128 - rank + k, lanes == 128 - rank + k + 1

            def pick(mask, v):
                return jnp.sum(jnp.where(mask, v, 0.0), axis=1, keepdims=True)

            m = inv_ref[...]
            row0, row1 = inv_ref[pl.ds(k, 1), :], inv_ref[pl.ds(k + 1, 1), :]
            col0, col1 = pick(at0, m), pick(at1, m)
            a, b = pick(at0[0:1], row0), pick(at1[0:1], row0)
            c, d = pick(at0[0:1], row1), pick(at1[0:1], row1)
            ratio = b / a
            row0 = row0 / a
            row1 = (row1 - c * row0) / (d - c * ratio)
            row0 = row0 - ratio * row1
            m = (m - col0 * row0) - col1 * row1
            m = jnp.where(rows == k, row0, m)
            inv_ref[...] = jnp.where(rows == k + 1, row1, m)
            return carry

        with jax.named_scope(f"eliminate{low}"):
            lax.fori_loop(low // 2, high // 2, step, 0)

    def wait_rows():
        with jax.named_scope("wait_bt"):
            pltpu.make_async_copy(bt_ref, bt_ref, local_sem.at[4]).wait()

    def gram_part(i, acc):
        c = i // 4
        z = lax.rem(i // 2, 2)
        x = lax.rem(i, 2) * 8
        flat = jnp.concatenate([bt_ref[c, z, x + k] for k in range(8)], axis=1)
        high = flat.astype(jnp.bfloat16)
        rest = flat - high.astype(F32)
        middle = rest.astype(jnp.bfloat16)
        low = (rest - middle.astype(F32)).astype(jnp.bfloat16)
        stacked = jnp.concatenate([high, middle, low], axis=0)
        return acc + lax.dot_general(
            stacked,
            stacked,
            (((1,), (1,)), ((), ())),
            preferred_element_type=F32,
        )

    each = rank // n_space

    def send_gram():
        with jax.named_scope("gram"):
            acc = lax.fori_loop(0, 16, gram_part, jnp.zeros((3 * rank, 3 * rank), F32))
        acc = acc[2 * rank :] + acc[rank : 2 * rank] + acc[:rank]
        gram = acc[:, 2 * rank :] + acc[:, rank : 2 * rank] + acc[:, :rank]
        gram = jnp.concatenate([jnp.zeros((rank, 128 - rank), F32), gram], axis=1)
        for o in range(n_space):
            gram_ref[0, o] = gram[o * each : o * each + each]
        gram_ref[1, s] = gram_ref[0, s]
        for j in far_first:
            send(
                gram_ref.at[0, at_s(j)], gram_ref.at[1, s], gram_sem.at[0], 0, j, gram_sem.at[2]
            )

    def wait_gram(k):
        with jax.named_scope(f"wait_gram{k}"):
            part = gram_ref.at[1, pl.ds(0, n_space - 1)]
            pltpu.make_async_copy(part, part, gram_sem.at[k]).wait()

    def share_gram():
        wait_gram(0)
        rows_sum = gram_ref[1, 0]
        for o in range(1, n_space):
            rows_sum = rows_sum + gram_ref[1, o]
        gram_ref[2, s] = rows_sum
        for j in far_first:
            send(
                gram_ref.at[2, s], gram_ref.at[2, s], gram_sem.at[1], 0, j, gram_sem.at[3]
            )

    with jax.named_scope("barrier"):
        pl.semaphore_wait(barrier, count)

    with jax.named_scope("wait_guess"):
        loads[0].wait()
    write_msg(msg_ref.at[R1], load_state(guess_ref))
    send_halo(R1, DEEP, 1)
    send_state(R1, guess_ref, 1)
    with jax.named_scope("wait_load12"):
        loads[1].wait()
        loads[2].wait()
    around = (
        ((slice(0, 2), slice(0, 2)), (slice(2, 3), slice(1, 2))),
        ((slice(0, 2), slice(0, 2)), (slice(2, 3), slice(0, 1))),
        ((slice(0, 1), slice(1, 2)),),
        ((slice(0, 1), slice(0, 1)),),
    )

    def part_of(cut):
        return pl.ds(cut.start, cut.stop - cut.start)

    def send_start(out):
        for k in (3, 2, 1, 0):
            if OFFSETS[k] in out:
                continue
            planes = part_of(around[k][0][1])
            pairs = [(speed_ref.at[planes], speed_halo.at[k, planes])]
            for steps_cut, planes_cut in around[k]:
                at = (part_of(steps_cut), part_of(planes_cut))
                pairs.append((force_ref.at[at], force_halo.at[(k, *at)]))
            for src, dst in pairs:
                send(src, dst, recv_sem.at[R1], 0, OFFSETS[k], None, out == ())

    where_it_is(send_start)

    wait_rows()
    send_gram()

    wait_round(R1, tuple((low, high + n) for (low, high), n in zip(DEEP, (7, 7, 2, 2))), 8)
    for j, value, on in (
        (0, speed_ref[0], None),
        (1, speed_ref[1], None),
        (-1, speed_halo[0, 1], e_dn1),
        (-2, speed_halo[0, 0], e_dn1),
        (2, speed_halo[1, 0], e_up1),
        (3, speed_halo[1, 1], e_up1),
        (-3, speed_halo[2, 1], e_dn2),
        (4, speed_halo[3, 0], e_up2),
    ):
        squared = value * value
        c2_ref[j + 3] = squared if on is None else squared * on

    def four_forced(i):
        state = load_state(own_ref.at[i])
        low, high = divergence(state)
        p, d = unpack(halo_of(i), state[0], (low, high), state[3][1], 4)
        values, _ = steps(p, d, DT, 4, forced=True)
        total = {
            j: (values[0][j] + values[1][j]) + (values[2][j] + values[3][j])
            for j in range(0, 3)
        }
        out = [[values[4][0], values[4][1]], [None] * 2, [None] * 2, [None] * 2]
        for z in range(2):
            for c, slope in enumerate(grad(total, z)):
                out[c + 1][z] = state[c + 1][z] - DT * slope
        return out

    relaxed = four_forced(R1)
    store_state(rel_ref, relaxed)
    write_msg(msg_ref.at[R2], relaxed)
    send_halo(R2, DEEP, 1)
    send_state(R2, rel_ref, 1)

    with jax.named_scope("wait_basis"):
        loads[3].wait()

    def column_msg(g, carry):
        for k in range(8):
            write_msg(bm_ref.at[g * 8 + k], load_state(b_ref.at[g * 8 + k]))
        return carry

    with jax.named_scope("column_msg"):
        lax.fori_loop(0, rank // 8, column_msg, 0)
    share_gram()
    wait_round(R2, DEEP, 8)
    residue = combine(lambda a, b: a - b, four_forced(R2), load_state(rel_ref))
    store_state(res_ref, residue)
    write_msg(msg_ref.at[R3], residue, deep=False)
    send(res_ref, own_ref.at[R3], recv_sem.at[ROUNDS], 1, 0)
    send_halo(R3, ONE, 1)


    def coarse(state, halo):
        p, d = unpack(halo, state[0], divergence(state), None, 1)
        values, _ = steps(p, d, 4 * DT, 1)
        out = [[values[1][0], values[1][1]], [None] * 2, [None] * 2, [None] * 2]
        for z in range(2):
            for c, slope in enumerate(grad(p, z)):
                out[c + 1][z] = state[c + 1][z] - (4 * DT) * slope
        return out

    def correction(halo, own):
        p, d = unpack(halo, (own[1], own[2]), (own[0], own[4]), own[3], 4)
        values, first = steps(p, d, DT, 4)
        moved = []
        for z in range(2):
            slow = p[z] - (4 * DT * c2(z)) * (d[z] - (4 * DT) * first[z])
            moved.append(values[4][z] - slow)
        total = {
            j: (values[1][j] - p[j]) + (values[2][j] - p[j]) + (values[3][j] - p[j])
            for j in range(0, 3)
        }
        dual = (DT * total[0], moved[0], moved[1], -DT * total[2], DT * total[1])
        for m in range(5):
            dual_ref[m] = dual[m]
        return moved, total

    def corrected(state, moved, total):
        out = [[state[0][z] + moved[z] for z in range(2)], [None] * 2, [None] * 2, [None] * 2]
        for z in range(2):
            for c, slope in enumerate(grad(total, z)):
                out[c + 1][z] = state[c + 1][z] - DT * slope
        return out

    def add(a, b):
        return a + b

    def candidate(n, i_y, i_x, x_state_ref):
        last = i_y == Y4
        if n == 0:
            invert_gram()
        wait_round(i_x, ONE, 0)
        z = combine(add, coarse(load_state(x_state_ref), halo_of(i_x)), load_state(res_ref))
        if last:
            store_state(fin_ref, combine(add, z, load_state(rel_ref)))
        else:
            store_state(zout_ref.at[n], z)
            send(zout_ref.at[n], zin_ref.at[n], recv_sem.at[ROUNDS + 1 + n], 1, 0)
        combine_columns(i_y, solved(n))
        send_halo(i_y, DEEP, 0 if last else 1)
        if last:
            full_products("products_last", fin_ref)
            wait_round(i_y, DEEP, 0)
            return correction(halo_of(i_y), msg_ref.at[i_y])
        send_own(i_y, msg_ref.at[i_y], yown_ref.at[n], 1)
        with jax.named_scope(f"wait_z{n}"):
            wait_planes(recv_sem.at[ROUNDS + 1 + n], 8)
        full_products(f"products_z{n}", zin_ref.at[n])
        wait_round(i_y, DEEP, 5)
        return correction(halo_of(i_y), yown_ref.at[n])

    def invert_gram():
        wait_gram(1)
        for o in range(n_space):
            inv_ref[o * each : o * each + each, :] = gram_ref[2, o]
        inv_ref[...] = inv_ref[...] + diagonal.astype(F32)
        eliminate(0, rank)

    def announce(i, state_ref, moved, total):
        msg_ref[i, 1] = state_ref[0, 0] + moved[0]
        msg_ref[i, 2] = state_ref[0, 1] + moved[1]
        msg_ref[i, 3] = state_ref[3, 1] - DT * (total[2] - total[1])
        send_halo(i, ONE, 0)

    with jax.named_scope("wait_res"):
        wait_planes(recv_sem.at[ROUNDS], 8)
    full_products("products0", own_ref.at[R3])
    share_products(0)
    for n, (i_y, i_x, ref) in enumerate(
        ((Y1, R3, own_ref.at[R3]), (Y2, X2, x_ref.at[0]))
    ):
        moved, total = candidate(n, i_y, i_x, ref)
        announce(X2 + n, zin_ref.at[n], moved, total)
        dual_products(f"products{n + 1}")
        share_products(n + 1)
        store_state(x_ref.at[n], corrected(load_state(zin_ref.at[n]), moved, total))
    moved, total = candidate(2, Y3, X3, x_ref.at[1])
    third = corrected(load_state(zin_ref.at[2]), moved, total)

    gap = combine(lambda a, b: a - b, third, load_state(x_ref.at[1]))
    store_state(gap_ref, gap)
    write_msg(msg_ref.at[GAP], gap)
    early = jnp.logical_and(t >= 1, t <= n_tm - 4)
    late = jnp.logical_or(t == 0, t >= n_tm - 3)

    @pl.when(early)
    def _():
        send_halo(GAP, TWO, 4, gap_sem.at[0])
        send_state(GAP, gap_ref, 4, gap_sem.at[0])

    store_state(x_ref.at[2], third)
    dual_products("products3")

    @pl.when(late)
    def _():
        wait_round(GAP, TWO, 8)
        state = load_state(own_ref.at[GAP])
        p, d = unpack(halo_of(GAP), state[0], divergence(state), state[3][1], 2)
        values, _ = steps(p, d, 8 * DT, 2)
        total = {j: values[0][j] + values[1][j] for j in range(0, 3)}
        behind = [[values[2][0], values[2][1]], [None] * 2, [None] * 2, [None] * 2]
        for z in range(2):
            for c, slope in enumerate(grad(total, z)):
                behind[c + 1][z] = state[c + 1][z] - (8 * DT) * slope
        store_state(x_ref.at[3], behind)
        store_state(x_ref.at[2], combine(add, load_state(x_ref.at[2]), behind))

    write_msg(msg_ref.at[X4], load_state(x_ref.at[2]), deep=False)
    send_halo(X4, ONE, 0)

    @pl.when(late)
    def _():
        full_products("products_gap", x_ref.at[3], True)

    share_products(3)
    moved, total = candidate(3, Y4, X4, x_ref.at[2])

    final = corrected(load_state(fin_ref), moved, total)
    store_state(fin_ref, final)
    write_msg(msg_ref.at[LAST], final)
    send_halo(LAST, THREE, 1)
    send_state(LAST, fin_ref, 1)
    dual_products("products4")
    share_products(4)
    store_state(states_ref.at[3], final)
    wait_round(LAST, THREE, 8)
    state = load_state(own_ref.at[LAST])
    p, d = unpack(halo_of(LAST), state[0], divergence(state), state[3][1], 3)
    values, _ = steps(p, d, DT, 3, forced=True)
    for n in range(3):
        for z in range(2):
            state[0][z] = values[n + 1][z]
            for c, slope in enumerate(grad(values[n], z)):
                state[c + 1][z] = state[c + 1][z] - DT * slope
        store_state(states_ref.at[n], state)
    coords_ref[...] = to_row(solved(4))[:, :rank]

    with jax.named_scope("wait_sends"):
        def wait_sent(out):
            total = sum(n for offset, n in sent.items() if offset not in out)
            planes, odd = divmod(total, math.prod(plane))
            assert odd == 0
            wait_planes(send_sem.at[0], planes)

        where_it_is(wait_sent)
        for k in (2, 3):
            wait_gram(k)
        for i in range(5):
            part = ar_ref.at[i, pl.ds(0, n_space - 1)]
            pltpu.make_async_copy(part, part, ar_send_sem.at[i]).wait()

        @pl.when(early)
        def _():
            def wait_gap(out):
                wait_planes(gap_sem.at[0], 8 + 4 * (1 not in out) + 3 * (-1 not in out))

            where_it_is(wait_gap)


def finish(states_ref, coords_ref, states_out, coords_out, sem):
    copies = [
        pltpu.make_async_copy(states_ref, states_out, sem.at[0]),
        pltpu.make_async_copy(coords_ref, coords_out, sem.at[1]),
    ]
    for copy in copies:
        copy.start()
    for copy in copies:
        copy.wait()


def body(n_tm, n_space, speed, forcing, guess, basis):
    rank = basis.shape[1]
    plane = speed.shape[1:]
    vmem = functools.partial(pltpu.VMEM, dtype=F32)
    dma = pltpu.SemaphoreType.DMA
    state = (4, 2, *plane)
    msg = (5, *plane)
    scratch = [
        vmem((rank, *state)),
        vmem((4, 2, plane[0], rank, plane[1])),
        vmem((rank, *msg)),
        vmem(state),
        vmem((2, *plane)),
        vmem((4, 2, *plane)),
        vmem((4, 2, *plane)),
        vmem((4, 3, 2, *plane)),
        vmem((8, *plane)),
        vmem((ROUNDS, *msg)),
        vmem((ROUNDS, 4, *msg)),
        vmem((ROUNDS, *state)),
        vmem((3, *msg)),
        vmem((4, *state)),
        vmem((3, *state)),
        vmem(state),
        vmem(state),
        vmem((4, *state)),
        vmem(state),
        vmem(state),
        vmem(msg),
        vmem((5, n_space, 1, 128)),
        vmem((3, n_space, rank // n_space, 128)),
        vmem((rank, 128)),
        vmem((rank, 128)),
        vmem((rank, 128)),
        dma((5,)),
        dma((1,)),
        dma((1,)),
        dma((ROUNDS + 4,)),
        dma((5,)),
        dma((5,)),
        dma((4,)),
    ]
    done = pl.pallas_call(
        functools.partial(kernel, n_tm, n_space, rank),
        out_shape=(
            pltpu.VMEM((4, *state), F32),
            pltpu.VMEM((1, rank), F32),
        ),
        in_specs=[pl.BlockSpec(memory_space=pl.ANY)] * 4,
        out_specs=(
            pl.BlockSpec(memory_space=pltpu.VMEM),
            pl.BlockSpec(memory_space=pltpu.VMEM),
        ),
        scratch_shapes=scratch,
        compiler_params=pltpu.CompilerParams(collective_id=0, has_side_effects=True),
    )(speed, forcing, guess, basis)
    return pl.pallas_call(
        finish,
        out_shape=(
            jax.ShapeDtypeStruct((4, *state), F32),
            jax.ShapeDtypeStruct((1, rank), F32),
        ),
        in_specs=[pl.BlockSpec(memory_space=pltpu.VMEM)] * 2,
        out_specs=[pl.BlockSpec(memory_space=pl.ANY)] * 2,
        scratch_shapes=[dma((2,))],
    )(*(pltpu.with_memory_space_constraint(v, pltpu.VMEM) for v in done))


def solution(mesh):
    placed = (
        P("space", None, None),
        P("tm", "space", None, None),
        P("tm", None, "space", None, None),
        P("tm", None, None, "space", None, None),
    )
    return jax.shard_map(
        functools.partial(body, mesh.shape["tm"], mesh.shape["space"]),
        mesh=mesh,
        in_specs=placed,
        out_specs=(P("tm", None, "space", None, None), P("tm", None)),
        check_vma=False,
    )
```

```python
import functools
import math

import jax
import jax.numpy as jnp
from jax import lax
from jax.experimental import pallas as pl
from jax.experimental.pallas import tpu as pltpu
from jax.sharding import PartitionSpec as P

DT = 0.045
MESH = pl.DeviceIdType.MESH
F32 = jnp.float32

R1, R2, R3, Y1, Y2, Y3, Y4, X2, X3, X4, GAP, LAST = range(12)
ROUNDS = 12

DEEP = ((0, 5), (0, 5), (1, 5), (0, 3))
THREE = ((0, 5), (0, 5), (2, 4), (1, 2))
TWO = ((2, 5), (0, 2))
ONE = ((2, 4), (1, 2))
OFFSETS = (1, -1, 2, -2)


def kernel(
    n_tm,
    n_space,
    rank,
    speed_hbm,
    forcing_hbm,
    guess_hbm,
    basis_hbm,
    states_ref,
    coords_ref,
    b_ref,
    bt_ref,
    bm_ref,
    guess_ref,
    speed_ref,
    force_ref,
    speed_halo,
    force_halo,
    c2_ref,
    msg_ref,
    halo_ref,
    own_ref,
    yown_ref,
    zout_ref,
    zin_ref,
    rel_ref,
    res_ref,
    x_ref,
    gap_ref,
    fin_ref,
    dual_ref,
    ar_ref,
    gram_ref,
    inv_ref,
    part_ref,
    w_ref,
    local_sem,
    send_sem,
    gap_sem,
    recv_sem,
    ar_send_sem,
    ar_sem,
    gram_sem,
):
    plane = guess_ref.shape[2:]
    t = lax.axis_index("tm")
    s = lax.axis_index("space")

    def at_t(d):
        return lax.rem(t + (d + n_tm), n_tm)

    def at_s(d):
        return lax.rem(s + (d + n_space), n_space)

    inner = jnp.logical_and(s >= 2, s <= n_space - 3)
    edge = jnp.logical_not(inner)
    has = {0: None, 1: s <= n_space - 2, -1: s >= 1, 2: s <= n_space - 3, -2: s >= 2}
    edges = ((0, (-1, -2)), (1, (-2,)), (n_space - 2, (2,)), (n_space - 1, (1, 2)))

    def where_it_is(act):
        @pl.when(inner)
        def _():
            act(())

        @pl.when(edge)
        def _():
            for place, out in edges:

                @pl.when(s == place)
                def _(out=out):
                    act(out)

    loads = [
        pltpu.make_async_copy(guess_hbm.at[0], guess_ref, local_sem.at[0]),
        pltpu.make_async_copy(speed_hbm, speed_ref, local_sem.at[1]),
        pltpu.make_async_copy(forcing_hbm, force_ref, local_sem.at[2]),
        pltpu.make_async_copy(basis_hbm.at[0], b_ref, local_sem.at[3]),
    ]
    for load in loads:
        load.start()

    far_first = sorted(range(1, n_space), key=lambda j: abs(abs(j - n_space // 2) - 2))

    def start_rows(m, carry):
        c = m // 2
        z = lax.rem(m, 2)
        for x in range(plane[0]):
            pltpu.make_async_copy(
                basis_hbm.at[0, :, c, z, x, :], bt_ref.at[c, z, x], local_sem.at[4]
            ).start()
        return carry

    barrier = pltpu.get_barrier_semaphore()
    count = 0
    with jax.named_scope("signals"):

        def greet(dt, ds):
            pl.semaphore_signal(
                barrier, inc=1, device_id=(at_t(dt), at_s(ds)), device_id_type=MESH
            )

        for ds in (2, -2, 1, -1, 0):
            near = (1, -1, 4) if abs(ds) < 2 else (1, -1)
            if has[ds] is None:
                count = count + len(near)
                for dt in near:
                    greet(dt, ds)
            else:
                count = count + len(near) * has[ds].astype(jnp.int32)

                @pl.when(has[ds])
                def _(near=near, ds=ds):
                    for dt in near:
                        greet(dt, ds)

        for ds in far_first:
            count = count + 1
            greet(0, ds)
    with jax.named_scope("rows"):
        lax.fori_loop(0, 8, start_rows, 0)

    sent = {offset: 0 for offset in has}

    def words(ref):
        return math.prod(ref.shape)

    def send(src, dst, rsem, dt, ds, ssem=None, tally=True):
        pltpu.make_async_remote_copy(
            src_ref=src,
            dst_ref=dst,
            send_sem=send_sem.at[0] if ssem is None else ssem,
            recv_sem=rsem,
            device_id=(at_t(dt), at_s(ds)),
            device_id_type=MESH,
        ).start()
        if ssem is None and tally:
            sent[ds] += words(src)

    def wait_planes(sem, planes):
        part = bm_ref.reshape(rank * 5, *plane).at[pl.ds(0, planes)]
        pltpu.make_async_copy(part, part, sem).wait()

    ix = lax.broadcasted_iota(jnp.int32, plane, 0)
    iy = lax.broadcasted_iota(jnp.int32, plane, 1)
    nx, ny = plane
    zero = jnp.zeros(plane, F32)
    x_low, x_high = ix == 0, ix == nx - 1
    y_low, y_high = iy == 0, iy == ny - 1
    weight = 5.0 - x_low.astype(F32) - y_low.astype(F32)

    def x_ahead(v):
        return jnp.where(x_high, zero, pltpu.roll(v, nx - 1, 0))

    def x_behind(v):
        return jnp.where(x_low, zero, pltpu.roll(v, 1, 0))

    def y_ahead(v):
        return jnp.where(y_high, zero, pltpu.roll(v, ny - 1, 1))

    def y_behind(v):
        return jnp.where(y_low, zero, pltpu.roll(v, 1, 1))

    def flag(cond):
        return jnp.where(cond, 1.0, 0.0).astype(F32)

    e_dn1, e_dn2 = flag(s >= 1), flag(s >= 2)
    e_up1, e_up2 = flag(s <= n_space - 2), flag(s <= n_space - 3)
    floor = {0: e_dn1, -2: e_dn2}

    def lap(p, j):
        below = p[j - 1] - p[j]
        if j in floor:
            below = below * floor[j]
        return (
            (x_ahead(p[j]) + x_behind(p[j]))
            + (y_ahead(p[j]) + y_behind(p[j]))
            + (p[j + 1] - weight * p[j])
            + below
        )

    def c2(j):
        return c2_ref[j + 3]

    def force(n, j):
        if j in (0, 1):
            return force_ref[n, j]
        if j in (-1, -2):
            return force_halo[0, n, j + 2] * e_dn1
        if j in (2, 3):
            return force_halo[1, n, j - 2] * e_up1
        if j == -3:
            return force_halo[2, 0, 1] * e_dn2
        return force_halo[3, 0, 0] * e_up2

    def steps(p, d, h, count, forced=False):
        values, first = [p], None
        for n in range(count):
            depth = count - 1 - n
            planes = range(-depth, 2 + depth)
            laps = {j: lap(p, j) for j in planes}
            if first is None:
                first = laps
            d = {j: d[j] - h * laps[j] for j in planes}
            p = {j: p[j] - (h * c2(j)) * d[j] for j in planes}
            if forced:
                p = {j: p[j] + force(n, j) for j in planes}
            values.append(p)
        return values, first

    def grad(p, j):
        return (x_ahead(p[j]) - p[j], y_ahead(p[j]) - p[j], p[j + 1] - p[j])

    def divergence(state):
        both = []
        for z in range(2):
            both.append(
                (state[1][z] - x_behind(state[1][z]))
                + (state[2][z] - y_behind(state[2][z]))
            )
        return both[0] + state[3][0], both[1] + (state[3][1] - state[3][0])

    def load_state(ref):
        return [[ref[c, z] for z in range(2)] for c in range(4)]

    def store_state(ref, state):
        for c in range(4):
            for z in range(2):
                ref[c, z] = state[c][z]

    def combine(fn, *states):
        return [[fn(*[u[c][z] for u in states]) for z in range(2)] for c in range(4)]

    def write_msg(ref, state, deep=True):
        if deep:
            low, high = divergence(state)
            ref[0] = low
            ref[4] = high
        ref[1] = state[0][0]
        ref[2] = state[0][1]
        ref[3] = state[3][1]

    def unpack(halo, own_p, own_d, own_vz, depth):
        p = {0: own_p[0], 1: own_p[1]}
        vz_below = halo[0, 3] * e_dn1
        p[-1] = halo[0, 2] * e_dn1
        p[2] = halo[1, 1] * e_up1
        d = {0: own_d[0] - vz_below, 1: own_d[1]}
        if depth >= 2:
            p[-2] = halo[0, 1] * e_dn1
            p[3] = halo[1, 2] * e_up1
            d[-1] = halo[0, 4]
            d[2] = halo[1, 0] - own_vz
        if depth >= 3:
            p[-3] = halo[2, 2] * e_dn2
            p[4] = halo[3, 1] * e_up2
            d[-2] = halo[0, 0] - halo[2, 3] * e_dn2
            d[3] = halo[1, 4]
        if depth >= 4:
            p[-4] = halo[2, 1] * e_dn2
            p[5] = halo[3, 2] * e_up2
            d[-3] = halo[2, 4]
            d[4] = halo[3, 0] - halo[1, 3]
        return p, d

    def send_halo(i, slices, dt, ssem=None):
        def act(out):
            for k in reversed(range(len(slices))):
                if OFFSETS[k] not in out:
                    low, high = slices[k]
                    part = pl.ds(low, high - low)
                    send(
                        msg_ref.at[i, part],
                        halo_ref.at[i, k, part],
                        recv_sem.at[i],
                        dt,
                        OFFSETS[k],
                        ssem,
                        out == (),
                    )

        where_it_is(act)

    def planes_of(slices, out=()):
        return sum(
            high - low for k, (low, high) in enumerate(slices) if -OFFSETS[k] not in out
        )

    def send_own(i, src, dst, dt, ssem=None):
        send(src, dst, recv_sem.at[i], dt, 0, ssem)

    def send_state(i, ref, dt, ssem=None):
        send_own(i, ref, own_ref.at[i], dt, ssem)

    def wait_round(i, slices, more):
        with jax.named_scope(f"wait_round{i}"):
            where_it_is(
                lambda out: wait_planes(recv_sem.at[i], planes_of(slices, out) + more)
            )

    def halo_of(i):
        return halo_ref.at[i]

    rows = lax.broadcasted_iota(jnp.int32, (rank, 128), 0)
    lanes = lax.broadcasted_iota(jnp.int32, (rank, 128), 1)
    diagonal = rows == lanes

    def to_row(column):
        spread = jnp.where(diagonal, jnp.broadcast_to(column, (rank, 128)), 0.0)
        return jnp.sum(spread, axis=0, keepdims=True)

    def products(name, columns, field, planes, more=False):
        with jax.named_scope(name):
            out = []
            for r in range(rank):
                total = None
                for at in planes:
                    for half in range(nx // 8):
                        part = (*at, slice(half * 8, half * 8 + 8), slice(None))
                        term = columns[(r, *part)] * field[part]
                        total = term if total is None else total + term
                out.append(jnp.sum(total, axis=0, keepdims=True))
                if r % 8 == 7:
                    block = jnp.concatenate(out, axis=0)
                    if more:
                        block = block + part_ref[r - 7 : r + 1, :]
                    part_ref[r - 7 : r + 1, :] = block
                    out = []

    def full_products(name, field, more=False):
        products(name, b_ref, field, [(c, z) for c in range(4) for z in range(2)], more)

    def dual_products(name):
        products(name, bm_ref, dual_ref, [(m,) for m in range(5)], True)

    def share_products(i):
        with jax.named_scope(f"share{i}"):
            ar_ref[i, s] = to_row(jnp.sum(part_ref[...], axis=1, keepdims=True))
            for j in far_first:
                send(ar_ref.at[i, s], ar_ref.at[i, s], ar_sem.at[i], 0, j, ar_send_sem.at[i])

    def solved(i):
        with jax.named_scope(f"wait_ar{i}"):
            part = ar_ref.at[i, pl.ds(0, n_space - 1)]
            pltpu.make_async_copy(part, part, ar_sem.at[i]).wait()
        total = ar_ref[i, 0]
        for j in range(1, n_space):
            total = total + ar_ref[i, j]
        return jnp.sum(inv_ref[...] * total, axis=1, keepdims=True)

    def combine_columns(i, weights):
        w_ref[...] = jnp.broadcast_to(weights, (rank, 128))

        def group(g, acc):
            for k in range(16):
                r = g * 16 + k
                w = jnp.broadcast_to(w_ref[pl.ds(r, 1), :], plane)
                acc = tuple(acc[m] + w * bm_ref[r, m] for m in range(5))
            return acc

        with jax.named_scope(f"columns{i}"):
            acc = lax.fori_loop(0, rank // 16, group, (zero,) * 5)
            for m in range(5):
                msg_ref[i, m] = acc[m]

    def eliminate(low, high):
        def step(i, carry):
            k = 2 * i
            at0, at1 = lanes == 128 - rank + k, lanes == 128 - rank + k + 1

            def pick(mask, v):
                return jnp.sum(jnp.where(mask, v, 0.0), axis=1, keepdims=True)

            m = inv_ref[...]
            row0, row1 = inv_ref[pl.ds(k, 1), :], inv_ref[pl.ds(k + 1, 1), :]
            col0, col1 = pick(at0, m), pick(at1, m)
            a, b = pick(at0[0:1], row0), pick(at1[0:1], row0)
            c, d = pick(at0[0:1], row1), pick(at1[0:1], row1)
            ratio = b / a
            row0 = row0 / a
            row1 = (row1 - c * row0) / (d - c * ratio)
            row0 = row0 - ratio * row1
            m = (m - col0 * row0) - col1 * row1
            m = jnp.where(rows == k, row0, m)
            inv_ref[...] = jnp.where(rows == k + 1, row1, m)
            return carry

        with jax.named_scope(f"eliminate{low}"):
            lax.fori_loop(low // 2, high // 2, step, 0)

    def wait_rows():
        with jax.named_scope("wait_bt"):
            pltpu.make_async_copy(bt_ref, bt_ref, local_sem.at[4]).wait()

    def gram_part(i, acc):
        c = i // 4
        z = lax.rem(i // 2, 2)
        x = lax.rem(i, 2) * 8
        flat = jnp.concatenate([bt_ref[c, z, x + k] for k in range(8)], axis=1)
        high = flat.astype(jnp.bfloat16)
        rest = flat - high.astype(F32)
        middle = rest.astype(jnp.bfloat16)
        low = (rest - middle.astype(F32)).astype(jnp.bfloat16)
        stacked = jnp.concatenate([high, middle, low], axis=0)
        return acc + lax.dot_general(
            stacked[: 2 * rank],
            stacked,
            (((1,), (1,)), ((), ())),
            preferred_element_type=F32,
        )

    each = rank // n_space

    def send_gram():
        with jax.named_scope("gram"):
            acc = lax.fori_loop(0, 16, gram_part, jnp.zeros((2 * rank, 3 * rank), F32))
        acc = acc[rank:] + acc[:rank]
        corner = acc[:, 2 * rank :]
        gram = (corner + corner.T) + acc[:, rank : 2 * rank] + acc[:, :rank]
        gram = jnp.concatenate([jnp.zeros((rank, 128 - rank), F32), gram], axis=1)
        for o in range(n_space):
            gram_ref[0, o] = gram[o * each : o * each + each]
        gram_ref[1, s] = gram_ref[0, s]
        for j in far_first:
            send(
                gram_ref.at[0, at_s(j)], gram_ref.at[1, s], gram_sem.at[0], 0, j, gram_sem.at[2]
            )

    def wait_gram(k):
        with jax.named_scope(f"wait_gram{k}"):
            part = gram_ref.at[1, pl.ds(0, n_space - 1)]
            pltpu.make_async_copy(part, part, gram_sem.at[k]).wait()

    def share_gram():
        wait_gram(0)
        rows_sum = gram_ref[1, 0]
        for o in range(1, n_space):
            rows_sum = rows_sum + gram_ref[1, o]
        gram_ref[2, s] = rows_sum
        for j in far_first:
            send(
                gram_ref.at[2, s], gram_ref.at[2, s], gram_sem.at[1], 0, j, gram_sem.at[3]
            )

    with jax.named_scope("barrier"):
        pl.semaphore_wait(barrier, count)

    with jax.named_scope("wait_guess"):
        loads[0].wait()
    write_msg(msg_ref.at[R1], load_state(guess_ref))
    with jax.named_scope("wait_load12"):
        loads[1].wait()
        loads[2].wait()
    around = (
        ((slice(0, 2), slice(0, 2)), (slice(2, 3), slice(1, 2))),
        ((slice(0, 2), slice(0, 2)), (slice(2, 3), slice(0, 1))),
        ((slice(0, 1), slice(1, 2)),),
        ((slice(0, 1), slice(0, 1)),),
    )

    def part_of(cut):
        return pl.ds(cut.start, cut.stop - cut.start)

    def send_start(out):
        for k in (3, 2, 1, 0):
            if OFFSETS[k] in out:
                continue
            part = part_of(slice(*DEEP[k]))
            send(
                msg_ref.at[R1, part],
                halo_ref.at[R1, k, part],
                recv_sem.at[R1],
                1,
                OFFSETS[k],
                None,
                out == (),
            )
            planes = part_of(around[k][0][1])
            pairs = [(speed_ref.at[planes], speed_halo.at[k, planes])]
            for steps_cut, planes_cut in around[k]:
                at = (part_of(steps_cut), part_of(planes_cut))
                pairs.append((force_ref.at[at], force_halo.at[(k, *at)]))
            for src, dst in pairs:
                send(src, dst, recv_sem.at[R1], 0, OFFSETS[k], None, out == ())

    where_it_is(send_start)
    send_state(R1, guess_ref, 1)

    def clear(out):
        for k in range(4):
            if -OFFSETS[k] in out:

                def clear_round(i, carry, k=k):
                    for m in range(5):
                        halo_ref[i, k, m] = zero
                    return carry

                lax.fori_loop(0, ROUNDS, clear_round, 0)
                for z in range(2):
                    speed_halo[k, z] = zero
                    for n in range(3):
                        force_halo[k, n, z] = zero

    where_it_is(clear)

    wait_rows()
    send_gram()

    wait_round(R1, tuple((low, high + n) for (low, high), n in zip(DEEP, (7, 7, 2, 2))), 8)
    for j, value, on in (
        (0, speed_ref[0], None),
        (1, speed_ref[1], None),
        (-1, speed_halo[0, 1], e_dn1),
        (-2, speed_halo[0, 0], e_dn1),
        (2, speed_halo[1, 0], e_up1),
        (3, speed_halo[1, 1], e_up1),
        (-3, speed_halo[2, 1], e_dn2),
        (4, speed_halo[3, 0], e_up2),
    ):
        squared = value * value
        c2_ref[j + 3] = squared if on is None else squared * on

    def four_forced(i):
        state = load_state(own_ref.at[i])
        low, high = divergence(state)
        p, d = unpack(halo_of(i), state[0], (low, high), state[3][1], 4)
        values, _ = steps(p, d, DT, 4, forced=True)
        total = {
            j: (values[0][j] + values[1][j]) + (values[2][j] + values[3][j])
            for j in range(0, 3)
        }
        out = [[values[4][0], values[4][1]], [None] * 2, [None] * 2, [None] * 2]
        for z in range(2):
            for c, slope in enumerate(grad(total, z)):
                out[c + 1][z] = state[c + 1][z] - DT * slope
        return out

    relaxed = four_forced(R1)
    store_state(rel_ref, relaxed)
    write_msg(msg_ref.at[R2], relaxed)
    send_halo(R2, DEEP, 1)
    send_state(R2, rel_ref, 1)

    with jax.named_scope("wait_basis"):
        loads[3].wait()

    def column_msg(g, carry):
        for k in range(8):
            write_msg(bm_ref.at[g * 8 + k], load_state(b_ref.at[g * 8 + k]))
        return carry

    with jax.named_scope("column_msg"):
        lax.fori_loop(0, rank // 8, column_msg, 0)
    share_gram()
    wait_round(R2, DEEP, 8)
    residue = combine(lambda a, b: a - b, four_forced(R2), load_state(rel_ref))
    store_state(res_ref, residue)
    write_msg(msg_ref.at[R3], residue, deep=False)
    send(res_ref, own_ref.at[R3], recv_sem.at[ROUNDS], 1, 0)
    send_halo(R3, ONE, 1)


    def coarse(state, halo):
        p, d = unpack(halo, state[0], divergence(state), None, 1)
        values, _ = steps(p, d, 4 * DT, 1)
        out = [[values[1][0], values[1][1]], [None] * 2, [None] * 2, [None] * 2]
        for z in range(2):
            for c, slope in enumerate(grad(p, z)):
                out[c + 1][z] = state[c + 1][z] - (4 * DT) * slope
        return out

    def correction(halo, own):
        p, d = unpack(halo, (own[1], own[2]), (own[0], own[4]), own[3], 4)
        values, first = steps(p, d, DT, 4)
        moved = []
        for z in range(2):
            slow = p[z] - (4 * DT * c2(z)) * (d[z] - (4 * DT) * first[z])
            moved.append(values[4][z] - slow)
        total = {
            j: (values[1][j] - p[j]) + (values[2][j] - p[j]) + (values[3][j] - p[j])
            for j in range(0, 3)
        }
        dual = (DT * total[0], moved[0], moved[1], -DT * total[2], DT * total[1])
        for m in range(5):
            dual_ref[m] = dual[m]
        return moved, total

    def corrected(state, moved, total):
        out = [[state[0][z] + moved[z] for z in range(2)], [None] * 2, [None] * 2, [None] * 2]
        for z in range(2):
            for c, slope in enumerate(grad(total, z)):
                out[c + 1][z] = state[c + 1][z] - DT * slope
        return out

    def write_edges(ref, state):
        h, p = 8 * DT, state[0]
        low, high = divergence(state)
        none = {-1: zero, 0: p[0], 1: p[1], 2: zero}

        def inside(j):
            return (
                (x_ahead(p[j]) + x_behind(p[j]))
                + (y_ahead(p[j]) + y_behind(p[j]))
                + (none[j + 1] - weight * p[j])
                + (none[j - 1] - p[j])
            )

        ref[0] = p[0] - (h * c2(0)) * (low - h * inside(0))
        ref[4] = p[1] - (h * c2(1)) * (high - h * inside(1))
        ref[1] = p[0]
        ref[2] = p[1]
        ref[3] = state[3][1]

    def two_steps(state, halo):
        h = 8 * DT
        low, high = divergence(state)
        p = {0: state[0][0], 1: state[0][1], -1: halo[0, 2] * e_dn1, 2: halo[1, 1] * e_up1}
        d = {0: low - halo[0, 3] * e_dn1, 1: high}
        values = [p]
        for n in range(2):
            d = {j: d[j] - h * lap(p, j) for j in range(2)}
            after = {j: p[j] - (h * c2(j)) * d[j] for j in range(2)}
            if n == 0:
                after[-1] = halo[0, 4] * e_dn1 + (h * h * c2(-1)) * p[0]
                after[2] = halo[1, 0] * e_up1 + (h * c2(2)) * (state[3][1] + h * p[1])
            p = after
            values.append(p)
        return values

    def add(a, b):
        return a + b

    def candidate(n, i_y, i_x, x_state_ref):
        last = i_y == Y4
        if n == 0:
            invert_gram()
        wait_round(i_x, ONE, 0)
        z = combine(add, coarse(load_state(x_state_ref), halo_of(i_x)), load_state(res_ref))
        if last:
            store_state(fin_ref, combine(add, z, load_state(rel_ref)))
        else:
            store_state(zout_ref.at[n], z)
            send(zout_ref.at[n], zin_ref.at[n], recv_sem.at[ROUNDS + 1 + n], 1, 0)
        combine_columns(i_y, solved(n))
        send_halo(i_y, DEEP, 0 if last else 1)
        if last:
            full_products("products_last", fin_ref)
            wait_round(i_y, DEEP, 0)
            return correction(halo_of(i_y), msg_ref.at[i_y])
        send_own(i_y, msg_ref.at[i_y], yown_ref.at[n], 1)
        with jax.named_scope(f"wait_z{n}"):
            wait_planes(recv_sem.at[ROUNDS + 1 + n], 8)
        full_products(f"products_z{n}", zin_ref.at[n])
        wait_round(i_y, DEEP, 5)
        return correction(halo_of(i_y), yown_ref.at[n])

    def invert_gram():
        wait_gram(1)
        for o in range(n_space):
            inv_ref[o * each : o * each + each, :] = gram_ref[2, o]
        inv_ref[...] = inv_ref[...] + diagonal.astype(F32)
        eliminate(0, rank)

    def announce(i, state_ref, moved, total):
        msg_ref[i, 1] = state_ref[0, 0] + moved[0]
        msg_ref[i, 2] = state_ref[0, 1] + moved[1]
        msg_ref[i, 3] = state_ref[3, 1] - DT * (total[2] - total[1])
        send_halo(i, ONE, 0)

    with jax.named_scope("wait_res"):
        wait_planes(recv_sem.at[ROUNDS], 8)
    full_products("products0", own_ref.at[R3])
    share_products(0)
    for n, (i_y, i_x, ref) in enumerate(
        ((Y1, R3, own_ref.at[R3]), (Y2, X2, x_ref.at[0]))
    ):
        moved, total = candidate(n, i_y, i_x, ref)
        dual_products(f"products{n + 1}")
        share_products(n + 1)
        announce(X2 + n, zin_ref.at[n], moved, total)
        store_state(x_ref.at[n], corrected(load_state(zin_ref.at[n]), moved, total))
    moved, total = candidate(2, Y3, X3, x_ref.at[1])
    third = corrected(load_state(zin_ref.at[2]), moved, total)

    gap = combine(lambda a, b: a - b, third, load_state(x_ref.at[1]))
    store_state(gap_ref, gap)
    write_edges(msg_ref.at[GAP], gap)
    early = jnp.logical_and(t >= 1, t <= n_tm - 4)
    late = jnp.logical_or(t == 0, t >= n_tm - 3)

    @pl.when(early)
    def _():
        send_halo(GAP, TWO, 4, gap_sem.at[0])
        send_state(GAP, gap_ref, 4, gap_sem.at[0])

    store_state(x_ref.at[2], third)
    dual_products("products3")

    @pl.when(late)
    def _():
        wait_round(GAP, TWO, 8)
        state = load_state(own_ref.at[GAP])
        values = two_steps(state, halo_of(GAP))
        total = {j: values[0][j] + values[1][j] for j in range(0, 3)}
        behind = [[values[2][0], values[2][1]], [None] * 2, [None] * 2, [None] * 2]
        for z in range(2):
            for c, slope in enumerate(grad(total, z)):
                behind[c + 1][z] = state[c + 1][z] - (8 * DT) * slope
        store_state(x_ref.at[3], behind)
        full_products("products_gap", x_ref.at[3], True)
        store_state(x_ref.at[2], combine(add, load_state(x_ref.at[2]), behind))

    share_products(3)
    write_msg(msg_ref.at[X4], load_state(x_ref.at[2]), deep=False)
    send_halo(X4, ONE, 0)
    moved, total = candidate(3, Y4, X4, x_ref.at[2])

    dual_products("products4")
    share_products(4)

    final = corrected(load_state(fin_ref), moved, total)
    store_state(fin_ref, final)
    write_msg(msg_ref.at[LAST], final)
    send_halo(LAST, THREE, 1)
    send_state(LAST, fin_ref, 1)
    store_state(states_ref.at[3], final)
    wait_round(LAST, THREE, 8)
    state = load_state(own_ref.at[LAST])
    p, d = unpack(halo_of(LAST), state[0], divergence(state), state[3][1], 3)
    values, _ = steps(p, d, DT, 3, forced=True)
    for n in range(3):
        for z in range(2):
            state[0][z] = values[n + 1][z]
            for c, slope in enumerate(grad(values[n], z)):
                state[c + 1][z] = state[c + 1][z] - DT * slope
        store_state(states_ref.at[n], state)
    coords_ref[...] = to_row(solved(4))[:, :rank]

    with jax.named_scope("wait_sends"):
        def wait_sent(out):
            total = sum(n for offset, n in sent.items() if offset not in out)
            planes, odd = divmod(total, math.prod(plane))
            assert odd == 0
            wait_planes(send_sem.at[0], planes)

        where_it_is(wait_sent)
        for k in (2, 3):
            wait_gram(k)
        for i in range(5):
            part = ar_ref.at[i, pl.ds(0, n_space - 1)]
            pltpu.make_async_copy(part, part, ar_send_sem.at[i]).wait()

        @pl.when(early)
        def _():
            def wait_gap(out):
                wait_planes(gap_sem.at[0], 8 + 3 * (1 not in out) + 2 * (-1 not in out))

            where_it_is(wait_gap)


def finish(states_ref, coords_ref, states_out, coords_out, sem):
    copies = [
        pltpu.make_async_copy(states_ref, states_out, sem.at[0]),
        pltpu.make_async_copy(coords_ref, coords_out, sem.at[1]),
    ]
    for copy in copies:
        copy.start()
    for copy in copies:
        copy.wait()


def body(n_tm, n_space, speed, forcing, guess, basis):
    rank = basis.shape[1]
    plane = speed.shape[1:]
    vmem = functools.partial(pltpu.VMEM, dtype=F32)
    dma = pltpu.SemaphoreType.DMA
    state = (4, 2, *plane)
    msg = (5, *plane)
    scratch = [
        vmem((rank, *state)),
        vmem((4, 2, plane[0], rank, plane[1])),
        vmem((rank, *msg)),
        vmem(state),
        vmem((2, *plane)),
        vmem((4, 2, *plane)),
        vmem((4, 2, *plane)),
        vmem((4, 3, 2, *plane)),
        vmem((8, *plane)),
        vmem((ROUNDS, *msg)),
        vmem((ROUNDS, 4, *msg)),
        vmem((ROUNDS, *state)),
        vmem((3, *msg)),
        vmem((4, *state)),
        vmem((3, *state)),
        vmem(state),
        vmem(state),
        vmem((4, *state)),
        vmem(state),
        vmem(state),
        vmem(msg),
        vmem((5, n_space, 1, 128)),
        vmem((3, n_space, rank // n_space, 128)),
        vmem((rank, 128)),
        vmem((rank, 128)),
        vmem((rank, 128)),
        dma((5,)),
        dma((1,)),
        dma((1,)),
        dma((ROUNDS + 4,)),
        dma((5,)),
        dma((5,)),
        dma((4,)),
    ]
    done = pl.pallas_call(
        functools.partial(kernel, n_tm, n_space, rank),
        out_shape=(
            pltpu.VMEM((4, *state), F32),
            pltpu.VMEM((1, rank), F32),
        ),
        in_specs=[pl.BlockSpec(memory_space=pl.ANY)] * 4,
        out_specs=(
            pl.BlockSpec(memory_space=pltpu.VMEM),
            pl.BlockSpec(memory_space=pltpu.VMEM),
        ),
        scratch_shapes=scratch,
        compiler_params=pltpu.CompilerParams(collective_id=0, has_side_effects=True),
    )(speed, forcing, guess, basis)
    return pl.pallas_call(
        finish,
        out_shape=(
            jax.ShapeDtypeStruct((4, *state), F32),
            jax.ShapeDtypeStruct((1, rank), F32),
        ),
        in_specs=[pl.BlockSpec(memory_space=pltpu.VMEM)] * 2,
        out_specs=[pl.BlockSpec(memory_space=pl.ANY)] * 2,
        scratch_shapes=[dma((2,))],
    )(*(pltpu.with_memory_space_constraint(v, pltpu.VMEM) for v in done))


def solution(mesh):
    placed = (
        P("space", None, None),
        P("tm", "space", None, None),
        P("tm", None, "space", None, None),
        P("tm", None, None, "space", None, None),
    )
    return jax.shard_map(
        functools.partial(body, mesh.shape["tm"], mesh.shape["space"]),
        mesh=mesh,
        in_specs=placed,
        out_specs=(P("tm", None, "space", None, None), P("tm", None)),
        check_vma=False,
    )
```

```python
import functools
import math

import jax
import jax.numpy as jnp
from jax import lax
from jax.experimental import pallas as pl
from jax.experimental.pallas import tpu as pltpu
from jax.sharding import PartitionSpec as P

DT = 0.045
MESH = pl.DeviceIdType.MESH
F32 = jnp.float32

R1, R2, R3, Y1, Y2, Y3, Y4, X2, X3, X4, GAP, LAST = range(12)
ROUNDS = 12

DEEP = ((0, 5), (0, 5), (1, 5), (0, 3))
THREE = ((0, 5), (0, 5), (2, 4), (1, 2))
TWO = ((2, 5), (0, 2))
ONE = ((2, 4), (1, 2))
OFFSETS = (1, -1, 2, -2)


def kernel(
    n_tm,
    n_space,
    rank,
    speed_hbm,
    forcing_hbm,
    guess_hbm,
    basis_hbm,
    states_ref,
    coords_ref,
    b_ref,
    bt_ref,
    bm_ref,
    guess_ref,
    speed_ref,
    force_ref,
    speed_halo,
    force_halo,
    c2_ref,
    msg_ref,
    halo_ref,
    own_ref,
    yown_ref,
    zout_ref,
    zin_ref,
    rel_ref,
    res_ref,
    x_ref,
    gap_ref,
    fin_ref,
    dual_ref,
    ar_ref,
    gram_ref,
    inv_ref,
    part_ref,
    w_ref,
    local_sem,
    send_sem,
    gap_sem,
    recv_sem,
    ar_send_sem,
    ar_sem,
    gram_sem,
):
    plane = guess_ref.shape[2:]
    t = lax.axis_index("tm")
    s = lax.axis_index("space")

    def at_t(d):
        return lax.rem(t + (d + n_tm), n_tm)

    def at_s(d):
        return lax.rem(s + (d + n_space), n_space)

    inner = jnp.logical_and(s >= 2, s <= n_space - 3)
    edge = jnp.logical_not(inner)
    has = {0: None, 1: s <= n_space - 2, -1: s >= 1, 2: s <= n_space - 3, -2: s >= 2}
    edges = ((0, (-1, -2)), (1, (-2,)), (n_space - 2, (2,)), (n_space - 1, (1, 2)))

    def where_it_is(act):
        @pl.when(inner)
        def _():
            act(())

        @pl.when(edge)
        def _():
            for place, out in edges:

                @pl.when(s == place)
                def _(out=out):
                    act(out)

    loads = [
        pltpu.make_async_copy(guess_hbm.at[0], guess_ref, local_sem.at[0]),
        pltpu.make_async_copy(speed_hbm, speed_ref, local_sem.at[1]),
        pltpu.make_async_copy(forcing_hbm, force_ref, local_sem.at[2]),
        pltpu.make_async_copy(basis_hbm.at[0], b_ref, local_sem.at[3]),
    ]
    for load in loads:
        load.start()

    far_first = sorted(range(1, n_space), key=lambda j: abs(abs(j - n_space // 2) - 2))

    def start_rows(m, carry):
        c = m // 2
        z = lax.rem(m, 2)
        for x in range(plane[0]):
            pltpu.make_async_copy(
                basis_hbm.at[0, :, c, z, x, :], bt_ref.at[c, z, x], local_sem.at[4]
            ).start()
        return carry

    barrier = pltpu.get_barrier_semaphore()
    count = 0
    with jax.named_scope("signals"):

        def greet(dt, ds):
            pl.semaphore_signal(
                barrier, inc=1, device_id=(at_t(dt), at_s(ds)), device_id_type=MESH
            )

        for ds in (2, -2, 1, -1, 0):
            near = (1, -1, 4) if abs(ds) < 2 else (1, -1)
            if has[ds] is None:
                count = count + len(near)
                for dt in near:
                    greet(dt, ds)
            else:
                count = count + len(near) * has[ds].astype(jnp.int32)

                @pl.when(has[ds])
                def _(near=near, ds=ds):
                    for dt in near:
                        greet(dt, ds)

        for ds in far_first:
            count = count + 1
            greet(0, ds)
    with jax.named_scope("rows"):
        lax.fori_loop(0, 8, start_rows, 0)

    sent = {offset: 0 for offset in has}

    def words(ref):
        return math.prod(ref.shape)

    def send(src, dst, rsem, dt, ds, ssem=None, tally=True):
        pltpu.make_async_remote_copy(
            src_ref=src,
            dst_ref=dst,
            send_sem=send_sem.at[0] if ssem is None else ssem,
            recv_sem=rsem,
            device_id=(at_t(dt), at_s(ds)),
            device_id_type=MESH,
        ).start()
        if ssem is None and tally:
            sent[ds] += words(src)

    def wait_planes(sem, planes):
        part = bm_ref.reshape(rank * 5, *plane).at[pl.ds(0, planes)]
        pltpu.make_async_copy(part, part, sem).wait()

    ix = lax.broadcasted_iota(jnp.int32, plane, 0)
    iy = lax.broadcasted_iota(jnp.int32, plane, 1)
    nx, ny = plane
    zero = jnp.zeros(plane, F32)
    x_low, x_high = ix == 0, ix == nx - 1
    y_low, y_high = iy == 0, iy == ny - 1
    weight = 5.0 - x_low.astype(F32) - y_low.astype(F32)

    def x_ahead(v):
        return jnp.where(x_high, zero, pltpu.roll(v, nx - 1, 0))

    def x_behind(v):
        return jnp.where(x_low, zero, pltpu.roll(v, 1, 0))

    def y_ahead(v):
        return jnp.where(y_high, zero, pltpu.roll(v, ny - 1, 1))

    def y_behind(v):
        return jnp.where(y_low, zero, pltpu.roll(v, 1, 1))

    def flag(cond):
        return jnp.where(cond, 1.0, 0.0).astype(F32)

    e_dn1, e_dn2 = flag(s >= 1), flag(s >= 2)
    e_up1, e_up2 = flag(s <= n_space - 2), flag(s <= n_space - 3)
    floor = {0: e_dn1, -2: e_dn2}

    def lap(p, j):
        below = p[j - 1] - p[j]
        if j in floor:
            below = below * floor[j]
        return (
            (x_ahead(p[j]) + x_behind(p[j]))
            + (y_ahead(p[j]) + y_behind(p[j]))
            + (p[j + 1] - weight * p[j])
            + below
        )

    def c2(j):
        return c2_ref[j + 3]

    def force(n, j):
        if j in (0, 1):
            return force_ref[n, j]
        if j in (-1, -2):
            return force_halo[0, n, j + 2] * e_dn1
        if j in (2, 3):
            return force_halo[1, n, j - 2] * e_up1
        if j == -3:
            return force_halo[2, 0, 1] * e_dn2
        return force_halo[3, 0, 0] * e_up2

    def steps(p, d, h, count, forced=False):
        values, first = [p], None
        for n in range(count):
            depth = count - 1 - n
            planes = range(-depth, 2 + depth)
            laps = {j: lap(p, j) for j in planes}
            if first is None:
                first = laps
            d = {j: d[j] - h * laps[j] for j in planes}
            p = {j: p[j] - (h * c2(j)) * d[j] for j in planes}
            if forced:
                p = {j: p[j] + force(n, j) for j in planes}
            values.append(p)
        return values, first

    def grad(p, j):
        return (x_ahead(p[j]) - p[j], y_ahead(p[j]) - p[j], p[j + 1] - p[j])

    def divergence(state):
        both = []
        for z in range(2):
            both.append(
                (state[1][z] - x_behind(state[1][z]))
                + (state[2][z] - y_behind(state[2][z]))
            )
        return both[0] + state[3][0], both[1] + (state[3][1] - state[3][0])

    def load_state(ref):
        return [[ref[c, z] for z in range(2)] for c in range(4)]

    def store_state(ref, state):
        for c in range(4):
            for z in range(2):
                ref[c, z] = state[c][z]

    def combine(fn, *states):
        return [[fn(*[u[c][z] for u in states]) for z in range(2)] for c in range(4)]

    def write_msg(ref, state, deep=True):
        if deep:
            low, high = divergence(state)
            ref[0] = low
            ref[4] = high
        ref[1] = state[0][0]
        ref[2] = state[0][1]
        ref[3] = state[3][1]

    def unpack(halo, own_p, own_d, own_vz, depth):
        p = {0: own_p[0], 1: own_p[1]}
        vz_below = halo[0, 3] * e_dn1
        p[-1] = halo[0, 2] * e_dn1
        p[2] = halo[1, 1] * e_up1
        d = {0: own_d[0] - vz_below, 1: own_d[1]}
        if depth >= 2:
            p[-2] = halo[0, 1] * e_dn1
            p[3] = halo[1, 2] * e_up1
            d[-1] = halo[0, 4]
            d[2] = halo[1, 0] - own_vz
        if depth >= 3:
            p[-3] = halo[2, 2] * e_dn2
            p[4] = halo[3, 1] * e_up2
            d[-2] = halo[0, 0] - halo[2, 3] * e_dn2
            d[3] = halo[1, 4]
        if depth >= 4:
            p[-4] = halo[2, 1] * e_dn2
            p[5] = halo[3, 2] * e_up2
            d[-3] = halo[2, 4]
            d[4] = halo[3, 0] - halo[1, 3]
        return p, d

    def send_halo(i, slices, dt, ssem=None):
        def act(out):
            for k in reversed(range(len(slices))):
                if OFFSETS[k] not in out:
                    low, high = slices[k]
                    part = pl.ds(low, high - low)
                    send(
                        msg_ref.at[i, part],
                        halo_ref.at[i, k, part],
                        recv_sem.at[i],
                        dt,
                        OFFSETS[k],
                        ssem,
                        out == (),
                    )

        where_it_is(act)

    def planes_of(slices, out=()):
        return sum(
            high - low for k, (low, high) in enumerate(slices) if -OFFSETS[k] not in out
        )

    def send_own(i, src, dst, dt, ssem=None):
        send(src, dst, recv_sem.at[i], dt, 0, ssem)

    def send_state(i, ref, dt, ssem=None):
        send_own(i, ref, own_ref.at[i], dt, ssem)

    def wait_round(i, slices, more):
        with jax.named_scope(f"wait_round{i}"):
            where_it_is(
                lambda out: wait_planes(recv_sem.at[i], planes_of(slices, out) + more)
            )

    def halo_of(i):
        return halo_ref.at[i]

    rows = lax.broadcasted_iota(jnp.int32, (rank, 128), 0)
    lanes = lax.broadcasted_iota(jnp.int32, (rank, 128), 1)
    diagonal = rows == lanes

    def to_row(column):
        spread = jnp.where(diagonal, jnp.broadcast_to(column, (rank, 128)), 0.0)
        return jnp.sum(spread, axis=0, keepdims=True)

    def products(name, columns, field, planes, more=False):
        with jax.named_scope(name):
            out = []
            for r in range(rank):
                total = None
                for at in planes:
                    for half in range(nx // 8):
                        part = (*at, slice(half * 8, half * 8 + 8), slice(None))
                        term = columns[(r, *part)] * field[part]
                        total = term if total is None else total + term
                out.append(jnp.sum(total, axis=0, keepdims=True))
                if r % 8 == 7:
                    block = jnp.concatenate(out, axis=0)
                    if more:
                        block = block + part_ref[r - 7 : r + 1, :]
                    part_ref[r - 7 : r + 1, :] = block
                    out = []

    def full_products(name, field, more=False):
        products(name, b_ref, field, [(c, z) for c in range(4) for z in range(2)], more)

    def dual_products(name):
        products(name, bm_ref, dual_ref, [(m,) for m in range(5)], True)

    def share_products(i):
        with jax.named_scope(f"share{i}"):
            ar_ref[i, s] = to_row(jnp.sum(part_ref[...], axis=1, keepdims=True))
            for j in far_first:
                send(ar_ref.at[i, s], ar_ref.at[i, s], ar_sem.at[i], 0, j, ar_send_sem.at[i])

    def solved(i):
        with jax.named_scope(f"wait_ar{i}"):
            part = ar_ref.at[i, pl.ds(0, n_space - 1)]
            pltpu.make_async_copy(part, part, ar_sem.at[i]).wait()
        total = ar_ref[i, 0]
        for j in range(1, n_space):
            total = total + ar_ref[i, j]
        return jnp.sum(inv_ref[...] * total, axis=1, keepdims=True)

    def combine_columns(i, weights):
        w_ref[...] = jnp.broadcast_to(weights, (rank, 128))

        def group(g, acc):
            for k in range(32):
                r = g * 32 + k
                w = jnp.broadcast_to(w_ref[pl.ds(r, 1), :], plane)
                acc = tuple(acc[m] + w * bm_ref[r, m] for m in range(5))
            return acc

        with jax.named_scope(f"columns{i}"):
            acc = lax.fori_loop(0, rank // 32, group, (zero,) * 5)
            for m in range(5):
                msg_ref[i, m] = acc[m]

    def eliminate(low, high):
        def step(i, carry):
            k = 2 * i
            at0, at1 = lanes == 128 - rank + k, lanes == 128 - rank + k + 1

            def pick(mask, v):
                return jnp.sum(jnp.where(mask, v, 0.0), axis=1, keepdims=True)

            m = inv_ref[...]
            row0, row1 = inv_ref[pl.ds(k, 1), :], inv_ref[pl.ds(k + 1, 1), :]
            col0, col1 = pick(at0, m), pick(at1, m)
            a, b = pick(at0[0:1], row0), pick(at1[0:1], row0)
            c, d = pick(at0[0:1], row1), pick(at1[0:1], row1)
            ratio = b / a
            row0 = row0 / a
            row1 = (row1 - c * row0) / (d - c * ratio)
            row0 = row0 - ratio * row1
            m = (m - col0 * row0) - col1 * row1
            m = jnp.where(rows == k, row0, m)
            inv_ref[...] = jnp.where(rows == k + 1, row1, m)
            return carry

        with jax.named_scope(f"eliminate{low}"):
            lax.fori_loop(low // 2, high // 2, step, 0)

    def wait_rows():
        with jax.named_scope("wait_bt"):
            pltpu.make_async_copy(bt_ref, bt_ref, local_sem.at[4]).wait()

    def gram_part(i, acc):
        c = i // 4
        z = lax.rem(i // 2, 2)
        x = lax.rem(i, 2) * 8
        flat = jnp.concatenate([bt_ref[c, z, x + k] for k in range(8)], axis=1)
        high = flat.astype(jnp.bfloat16)
        rest = flat - high.astype(F32)
        middle = rest.astype(jnp.bfloat16)
        low = (rest - middle.astype(F32)).astype(jnp.bfloat16)
        stacked = jnp.concatenate([high, middle, low], axis=0)
        return acc + lax.dot_general(
            stacked[: 2 * rank],
            stacked,
            (((1,), (1,)), ((), ())),
            preferred_element_type=F32,
        )

    each = rank // n_space

    def send_gram():
        with jax.named_scope("gram"):
            acc = lax.fori_loop(0, 16, gram_part, jnp.zeros((2 * rank, 3 * rank), F32))
        acc = acc[rank:] + acc[:rank]
        corner = acc[:, 2 * rank :]
        gram = (corner + corner.T) + acc[:, rank : 2 * rank] + acc[:, :rank]
        gram = jnp.concatenate([jnp.zeros((rank, 128 - rank), F32), gram], axis=1)
        for o in range(n_space):
            gram_ref[0, o] = gram[o * each : o * each + each]
        gram_ref[1, s] = gram_ref[0, s]
        for j in far_first:
            send(
                gram_ref.at[0, at_s(j)], gram_ref.at[1, s], gram_sem.at[0], 0, j, gram_sem.at[2]
            )

    def wait_gram(k):
        with jax.named_scope(f"wait_gram{k}"):
            part = gram_ref.at[1, pl.ds(0, n_space - 1)]
            pltpu.make_async_copy(part, part, gram_sem.at[k]).wait()

    def share_gram():
        wait_gram(0)
        rows_sum = gram_ref[1, 0]
        for o in range(1, n_space):
            rows_sum = rows_sum + gram_ref[1, o]
        gram_ref[2, s] = rows_sum
        for j in far_first:
            send(
                gram_ref.at[2, s], gram_ref.at[2, s], gram_sem.at[1], 0, j, gram_sem.at[3]
            )

    with jax.named_scope("barrier"):
        pl.semaphore_wait(barrier, count)

    with jax.named_scope("wait_guess"):
        loads[0].wait()
    write_msg(msg_ref.at[R1], load_state(guess_ref))
    with jax.named_scope("wait_load12"):
        loads[1].wait()
        loads[2].wait()
    around = (
        ((slice(0, 2), slice(0, 2)), (slice(2, 3), slice(1, 2))),
        ((slice(0, 2), slice(0, 2)), (slice(2, 3), slice(0, 1))),
        ((slice(0, 1), slice(1, 2)),),
        ((slice(0, 1), slice(0, 1)),),
    )

    def part_of(cut):
        return pl.ds(cut.start, cut.stop - cut.start)

    def send_start(out):
        for k in (3, 2, 1, 0):
            if OFFSETS[k] in out:
                continue
            part = part_of(slice(*DEEP[k]))
            send(
                msg_ref.at[R1, part],
                halo_ref.at[R1, k, part],
                recv_sem.at[R1],
                1,
                OFFSETS[k],
                None,
                out == (),
            )
            planes = part_of(around[k][0][1])
            pairs = [(speed_ref.at[planes], speed_halo.at[k, planes])]
            for steps_cut, planes_cut in around[k]:
                at = (part_of(steps_cut), part_of(planes_cut))
                pairs.append((force_ref.at[at], force_halo.at[(k, *at)]))
            for src, dst in pairs:
                send(src, dst, recv_sem.at[R1], 0, OFFSETS[k], None, out == ())

    where_it_is(send_start)
    send_state(R1, guess_ref, 1)

    def clear(out):
        for k in range(4):
            if -OFFSETS[k] in out:

                def clear_round(i, carry, k=k):
                    for m in range(5):
                        halo_ref[i, k, m] = zero
                    return carry

                lax.fori_loop(0, ROUNDS, clear_round, 0)
                for z in range(2):
                    speed_halo[k, z] = zero
                    for n in range(3):
                        force_halo[k, n, z] = zero

    where_it_is(clear)

    wait_rows()
    send_gram()

    wait_round(R1, tuple((low, high + n) for (low, high), n in zip(DEEP, (7, 7, 2, 2))), 8)
    for j, value, on in (
        (0, speed_ref[0], None),
        (1, speed_ref[1], None),
        (-1, speed_halo[0, 1], e_dn1),
        (-2, speed_halo[0, 0], e_dn1),
        (2, speed_halo[1, 0], e_up1),
        (3, speed_halo[1, 1], e_up1),
        (-3, speed_halo[2, 1], e_dn2),
        (4, speed_halo[3, 0], e_up2),
    ):
        squared = value * value
        c2_ref[j + 3] = squared if on is None else squared * on

    def four_forced(i):
        state = load_state(own_ref.at[i])
        low, high = divergence(state)
        p, d = unpack(halo_of(i), state[0], (low, high), state[3][1], 4)
        values, _ = steps(p, d, DT, 4, forced=True)
        total = {
            j: (values[0][j] + values[1][j]) + (values[2][j] + values[3][j])
            for j in range(0, 3)
        }
        out = [[values[4][0], values[4][1]], [None] * 2, [None] * 2, [None] * 2]
        for z in range(2):
            for c, slope in enumerate(grad(total, z)):
                out[c + 1][z] = state[c + 1][z] - DT * slope
        return out

    relaxed = four_forced(R1)
    store_state(rel_ref, relaxed)
    write_msg(msg_ref.at[R2], relaxed)
    send_halo(R2, DEEP, 1)
    send_state(R2, rel_ref, 1)

    with jax.named_scope("wait_basis"):
        loads[3].wait()

    def column_msg(g, carry):
        for k in range(8):
            write_msg(bm_ref.at[g * 8 + k], load_state(b_ref.at[g * 8 + k]))
        return carry

    with jax.named_scope("column_msg"):
        lax.fori_loop(0, rank // 8, column_msg, 0)
    share_gram()
    wait_round(R2, DEEP, 8)
    residue = combine(lambda a, b: a - b, four_forced(R2), load_state(rel_ref))
    store_state(res_ref, residue)
    write_msg(msg_ref.at[R3], residue, deep=False)
    send(res_ref, own_ref.at[R3], recv_sem.at[ROUNDS], 1, 0)
    send_halo(R3, ONE, 1)


    def coarse(state, halo):
        p, d = unpack(halo, state[0], divergence(state), None, 1)
        values, _ = steps(p, d, 4 * DT, 1)
        out = [[values[1][0], values[1][1]], [None] * 2, [None] * 2, [None] * 2]
        for z in range(2):
            for c, slope in enumerate(grad(p, z)):
                out[c + 1][z] = state[c + 1][z] - (4 * DT) * slope
        return out

    def correction(halo, own):
        p, d = unpack(halo, (own[1], own[2]), (own[0], own[4]), own[3], 4)
        values, first = steps(p, d, DT, 4)
        moved = []
        for z in range(2):
            slow = p[z] - (4 * DT * c2(z)) * (d[z] - (4 * DT) * first[z])
            moved.append(values[4][z] - slow)
        total = {
            j: (values[1][j] - p[j]) + (values[2][j] - p[j]) + (values[3][j] - p[j])
            for j in range(0, 3)
        }
        dual = (DT * total[0], moved[0], moved[1], -DT * total[2], DT * total[1])
        for m in range(5):
            dual_ref[m] = dual[m]
        return moved, total

    def corrected(state, moved, total):
        out = [[state[0][z] + moved[z] for z in range(2)], [None] * 2, [None] * 2, [None] * 2]
        for z in range(2):
            for c, slope in enumerate(grad(total, z)):
                out[c + 1][z] = state[c + 1][z] - DT * slope
        return out

    def write_edges(ref, state):
        h, p = 8 * DT, state[0]
        low, high = divergence(state)
        none = {-1: zero, 0: p[0], 1: p[1], 2: zero}

        def inside(j):
            return (
                (x_ahead(p[j]) + x_behind(p[j]))
                + (y_ahead(p[j]) + y_behind(p[j]))
                + (none[j + 1] - weight * p[j])
                + (none[j - 1] - p[j])
            )

        ref[0] = p[0] - (h * c2(0)) * (low - h * inside(0))
        ref[4] = p[1] - (h * c2(1)) * (high - h * inside(1))
        ref[1] = p[0]
        ref[2] = p[1]
        ref[3] = state[3][1]

    def two_steps(state, halo):
        h = 8 * DT
        low, high = divergence(state)
        p = {0: state[0][0], 1: state[0][1], -1: halo[0, 2] * e_dn1, 2: halo[1, 1] * e_up1}
        d = {0: low - halo[0, 3] * e_dn1, 1: high}
        values = [p]
        for n in range(2):
            d = {j: d[j] - h * lap(p, j) for j in range(2)}
            after = {j: p[j] - (h * c2(j)) * d[j] for j in range(2)}
            if n == 0:
                after[-1] = halo[0, 4] * e_dn1 + (h * h * c2(-1)) * p[0]
                after[2] = halo[1, 0] * e_up1 + (h * c2(2)) * (state[3][1] + h * p[1])
            p = after
            values.append(p)
        return values

    def add(a, b):
        return a + b

    def candidate(n, i_y, i_x, x_state_ref):
        last = i_y == Y4
        if n == 0:
            invert_gram()
        wait_round(i_x, ONE, 0)
        z = combine(add, coarse(load_state(x_state_ref), halo_of(i_x)), load_state(res_ref))
        if last:
            store_state(fin_ref, combine(add, z, load_state(rel_ref)))
        else:
            store_state(zout_ref.at[n], z)
            send(zout_ref.at[n], zin_ref.at[n], recv_sem.at[ROUNDS + 1 + n], 1, 0)
        combine_columns(i_y, solved(n))
        send_halo(i_y, DEEP, 0 if last else 1)
        if last:
            full_products("products_last", fin_ref)
            wait_round(i_y, DEEP, 0)
            return correction(halo_of(i_y), msg_ref.at[i_y])
        send_own(i_y, msg_ref.at[i_y], yown_ref.at[n], 1)
        with jax.named_scope(f"wait_z{n}"):
            wait_planes(recv_sem.at[ROUNDS + 1 + n], 8)
        full_products(f"products_z{n}", zin_ref.at[n])
        wait_round(i_y, DEEP, 5)
        return correction(halo_of(i_y), yown_ref.at[n])

    def invert_gram():
        wait_gram(1)
        for o in range(n_space):
            inv_ref[o * each : o * each + each, :] = gram_ref[2, o]
        inv_ref[...] = inv_ref[...] + diagonal.astype(F32)
        eliminate(0, rank)

    def announce(i, state_ref, moved, total):
        msg_ref[i, 1] = state_ref[0, 0] + moved[0]
        msg_ref[i, 2] = state_ref[0, 1] + moved[1]
        msg_ref[i, 3] = state_ref[3, 1] - DT * (total[2] - total[1])
        send_halo(i, ONE, 0)

    with jax.named_scope("wait_res"):
        wait_planes(recv_sem.at[ROUNDS], 8)
    full_products("products0", own_ref.at[R3])
    share_products(0)
    for n, (i_y, i_x, ref) in enumerate(
        ((Y1, R3, own_ref.at[R3]), (Y2, X2, x_ref.at[0]))
    ):
        moved, total = candidate(n, i_y, i_x, ref)
        announce(X2 + n, zin_ref.at[n], moved, total)
        dual_products(f"products{n + 1}")
        share_products(n + 1)
        store_state(x_ref.at[n], corrected(load_state(zin_ref.at[n]), moved, total))
    moved, total = candidate(2, Y3, X3, x_ref.at[1])
    third = corrected(load_state(zin_ref.at[2]), moved, total)

    gap = combine(lambda a, b: a - b, third, load_state(x_ref.at[1]))
    store_state(gap_ref, gap)
    write_edges(msg_ref.at[GAP], gap)
    early = jnp.logical_and(t >= 1, t <= n_tm - 4)
    late = jnp.logical_or(t == 0, t >= n_tm - 3)

    @pl.when(early)
    def _():
        send_halo(GAP, TWO, 4, gap_sem.at[0])
        send_state(GAP, gap_ref, 4, gap_sem.at[0])

    store_state(x_ref.at[2], third)
    dual_products("products3")

    @pl.when(late)
    def _():
        wait_round(GAP, TWO, 8)
        state = load_state(own_ref.at[GAP])
        values = two_steps(state, halo_of(GAP))
        total = {j: values[0][j] + values[1][j] for j in range(0, 3)}
        behind = [[values[2][0], values[2][1]], [None] * 2, [None] * 2, [None] * 2]
        for z in range(2):
            for c, slope in enumerate(grad(total, z)):
                behind[c + 1][z] = state[c + 1][z] - (8 * DT) * slope
        store_state(x_ref.at[3], behind)
        full_products("products_gap", x_ref.at[3], True)
        store_state(x_ref.at[2], combine(add, load_state(x_ref.at[2]), behind))

    share_products(3)
    write_msg(msg_ref.at[X4], load_state(x_ref.at[2]), deep=False)
    send_halo(X4, ONE, 0)
    moved, total = candidate(3, Y4, X4, x_ref.at[2])

    dual_products("products4")
    share_products(4)

    final = corrected(load_state(fin_ref), moved, total)
    store_state(fin_ref, final)
    write_msg(msg_ref.at[LAST], final)
    send_halo(LAST, THREE, 1)
    send_state(LAST, fin_ref, 1)
    store_state(states_ref.at[3], final)
    wait_round(LAST, THREE, 8)
    state = load_state(own_ref.at[LAST])
    p, d = unpack(halo_of(LAST), state[0], divergence(state), state[3][1], 3)
    values, _ = steps(p, d, DT, 3, forced=True)
    for n in range(3):
        for z in range(2):
            state[0][z] = values[n + 1][z]
            for c, slope in enumerate(grad(values[n], z)):
                state[c + 1][z] = state[c + 1][z] - DT * slope
        store_state(states_ref.at[n], state)
    coords_ref[...] = to_row(solved(4))[:, :rank]

    with jax.named_scope("wait_sends"):
        def wait_sent(out):
            total = sum(n for offset, n in sent.items() if offset not in out)
            planes, odd = divmod(total, math.prod(plane))
            assert odd == 0
            wait_planes(send_sem.at[0], planes)

        where_it_is(wait_sent)
        for k in (2, 3):
            wait_gram(k)
        for i in range(5):
            part = ar_ref.at[i, pl.ds(0, n_space - 1)]
            pltpu.make_async_copy(part, part, ar_send_sem.at[i]).wait()

        @pl.when(early)
        def _():
            def wait_gap(out):
                wait_planes(gap_sem.at[0], 8 + 3 * (1 not in out) + 2 * (-1 not in out))

            where_it_is(wait_gap)


def finish(states_ref, coords_ref, states_out, coords_out, sem):
    copies = [
        pltpu.make_async_copy(states_ref, states_out, sem.at[0]),
        pltpu.make_async_copy(coords_ref, coords_out, sem.at[1]),
    ]
    for copy in copies:
        copy.start()
    for copy in copies:
        copy.wait()


def body(n_tm, n_space, speed, forcing, guess, basis):
    rank = basis.shape[1]
    plane = speed.shape[1:]
    vmem = functools.partial(pltpu.VMEM, dtype=F32)
    dma = pltpu.SemaphoreType.DMA
    state = (4, 2, *plane)
    msg = (5, *plane)
    scratch = [
        vmem((rank, *state)),
        vmem((4, 2, plane[0], rank, plane[1])),
        vmem((rank, *msg)),
        vmem(state),
        vmem((2, *plane)),
        vmem((4, 2, *plane)),
        vmem((4, 2, *plane)),
        vmem((4, 3, 2, *plane)),
        vmem((8, *plane)),
        vmem((ROUNDS, *msg)),
        vmem((ROUNDS, 4, *msg)),
        vmem((ROUNDS, *state)),
        vmem((3, *msg)),
        vmem((4, *state)),
        vmem((3, *state)),
        vmem(state),
        vmem(state),
        vmem((4, *state)),
        vmem(state),
        vmem(state),
        vmem(msg),
        vmem((5, n_space, 1, 128)),
        vmem((3, n_space, rank // n_space, 128)),
        vmem((rank, 128)),
        vmem((rank, 128)),
        vmem((rank, 128)),
        dma((5,)),
        dma((1,)),
        dma((1,)),
        dma((ROUNDS + 4,)),
        dma((5,)),
        dma((5,)),
        dma((4,)),
    ]
    done = pl.pallas_call(
        functools.partial(kernel, n_tm, n_space, rank),
        out_shape=(
            pltpu.VMEM((4, *state), F32),
            pltpu.VMEM((1, rank), F32),
        ),
        in_specs=[pl.BlockSpec(memory_space=pl.ANY)] * 4,
        out_specs=(
            pl.BlockSpec(memory_space=pltpu.VMEM),
            pl.BlockSpec(memory_space=pltpu.VMEM),
        ),
        scratch_shapes=scratch,
        compiler_params=pltpu.CompilerParams(collective_id=0, has_side_effects=True),
    )(speed, forcing, guess, basis)
    return pl.pallas_call(
        finish,
        out_shape=(
            jax.ShapeDtypeStruct((4, *state), F32),
            jax.ShapeDtypeStruct((1, rank), F32),
        ),
        in_specs=[pl.BlockSpec(memory_space=pltpu.VMEM)] * 2,
        out_specs=[pl.BlockSpec(memory_space=pl.ANY)] * 2,
        scratch_shapes=[dma((2,))],
    )(*(pltpu.with_memory_space_constraint(v, pltpu.VMEM) for v in done))


def solution(mesh):
    placed = (
        P("space", None, None),
        P("tm", "space", None, None),
        P("tm", None, "space", None, None),
        P("tm", None, None, "space", None, None),
    )
    return jax.shard_map(
        functools.partial(body, mesh.shape["tm"], mesh.shape["space"]),
        mesh=mesh,
        in_specs=placed,
        out_specs=(P("tm", None, "space", None, None), P("tm", None)),
        check_vma=False,
    )
```
